32 devices in a mesh: tok: 16 (over z, y, core), cand: 2 (over x).
Axes of the slice: x: 2, y: 2, z: 4, core: 2. Of those that a mesh axis runs over, the one named last changes fastest.
Arguments:
- dec_hidden: bfloat16 [2, 16, 32, 2048], P(None, 'cand'), may hold values from -6 to 6
- enc_keys: bfloat16 [2, 2048, 2048], P(None, 'tok'), may hold values from -250 to 250
- enc_values: bfloat16 [2, 2048, 2048], P(None, 'tok'), may hold values from -72 to 72
- enc_lengths: int32 [2], replicated, may hold values from 512 to 2048, as said below
- cand_counts: int32 [2], replicated, may hold values from 4 to 16, as said below
- gold_ids: int32 [2, 16, 32], P(None, 'cand'), may hold values from 0 to 32127
- gain_cross: float32 [2048], replicated, may hold values from 0.25 to 1.75
- w_query: bfloat16 [2048, 2048], P('cand', 'tok'), may hold values from -0.125 to 0.125
- w_out: bfloat16 [2048, 2048], P('tok', 'cand'), may hold values from -0.125 to 0.125
- gain_ffn: float32 [2048], replicated, may hold values from 0.25 to 1.75
- w_in_gate: bfloat16 [2048, 5120], P('cand', 'tok'), may hold values from -0.125 to 0.125
- w_in_up: bfloat16 [2048, 5120], P('cand', 'tok'), may hold values from -0.125 to 0.125
- w_ffn_out: bfloat16 [5120, 2048], P('tok', 'cand'), may hold values from -0.25 to 0.25
- gain_final: float32 [2048], replicated, may hold values from 0.25 to 1.75
- w_vocab: bfloat16 [2048, 32128], P('cand', 'tok'), may hold values from -20 to 20
Outputs:
- cand_scores: float32 [2, 16], P(None, 'cand')
- best_score: float32 [2], replicated
The draws below stay inside these ranges and needn't reach their ends.
Inputs may be any that keep to these rules, and one draw needn't show every extreme that they name: `enc_lengths`: some query has all 2048 encoder tokens live. `cand_counts`: some query has all 16 candidates live.
All inputs are finite; a program needn't handle non-finite values.
Results may differ from the reference program's by a relative error of at most 0.0014.
The reference program's roundings to bfloat16 on the way count: a program that leaves them out, or rounds other values in their place, can miss the bound.
Values may be sent and summed in bfloat16 or wider, within the bound.
No kernel may reach another device: no remote copies, remote signals or barrier semaphores. Data moves between devices by JAX's collectives and lax.ppermute only.
A program may use at most 64 MiB of HBM per device.

```python
import math
import jax
import jax.numpy as jnp
import numpy as np
from jax import lax

D = 2048
HEADS = 32
HEAD_DIM = 64
FF = 5120
VOCAB = 32128
QUERIES = 2
LENGTH = 32
CANDS = 16
SRC = 2048


def draw_enc_keys(key, part):
    base = 0.25 * jax.random.truncated_normal(key, -6.0, 6.0, (QUERIES, SRC, D), jnp.float32)
    return base.astype(jnp.bfloat16)


def draw_w_vocab(key, part):
    base = 4.0 * jax.random.truncated_normal(key, -6.0, 6.0, (D, VOCAB), jnp.float32) / jnp.sqrt(float(D))
    return jnp.clip(base, -20.0, 20.0).astype(jnp.bfloat16)


def draw_enc_lengths(key, part):
    drawn = jax.random.randint(key, (QUERIES,), SRC // 4, SRC + 1)
    chosen = jax.random.randint(jax.random.fold_in(key, 7), (), 0, QUERIES)
    return jnp.where(jnp.arange(QUERIES) == chosen, SRC, drawn).astype(jnp.int32)


def draw_cand_counts(key, part):
    drawn = jax.random.randint(key, (QUERIES,), CANDS // 4, CANDS + 1)
    chosen = jax.random.randint(jax.random.fold_in(key, 11), (), 0, QUERIES)
    return jnp.where(jnp.arange(QUERIES) == chosen, CANDS, drawn).astype(jnp.int32)


def set_ends(values, stream_key, smallest, largest):
    place = [jax.random.randint(jax.random.fold_in(stream_key, axis), (), 0, length) for axis, length in enumerate(values.shape)]
    longest = values.shape.index(max(values.shape))
    beside = place[:longest] + [(place[longest] + 1) % values.shape[longest]] + place[longest + 1:]
    return values.at[tuple(place)].set(smallest).at[tuple(beside)].set(largest)


def block_levels(own_key, dims, split, smallest, top_value):
    level, own = 1.0, jax.random.fold_in(own_key, 6)
    for axis_at, blocks in split:
        heights = jnp.exp(jax.random.uniform(jax.random.fold_in(own, axis_at), (blocks,), jnp.float32, smallest / len(split), top_value / len(split)))
        level = level * jnp.repeat(heights, dims[axis_at] // blocks).reshape([-1 if axis == axis_at else 1 for axis in range(len(dims))])
    return level


def rank_table(count, skew):
    portions = [(1 << 20) // math.isqrt(rank ** skew) + 1 for rank in range(1, count + 1)]
    width = 1 + sum(portions) // (1 << 30)
    return np.cumsum(np.array([max(1, weight // width) for weight in portions]))


def ranked(own_key, shape, number_of, slope):
    grid = rank_table(number_of, slope)
    lot = jax.random.randint(jax.random.fold_in(own_key, 1), shape, 0, int(grid[number_of - 1]))
    grade = jnp.searchsorted(jnp.asarray(grid, jnp.int32), lot, side="right")
    return jax.random.permutation(jax.random.fold_in(own_key, 2), number_of)[grade].astype(jnp.int32)


def centred(stream_key, extent, deviation, limit, shards=(), kind=jnp.bfloat16):
    values = jax.random.normal(stream_key, extent, jnp.float32) * deviation
    if len(shards) > 0:
        values = block_levels(stream_key, extent, shards, -0.22, 0.18) * values
    return jnp.clip(values, min=-limit, max=limit).astype(kind)


def setup_inputs(seed: int = 0) -> dict:
    keys = jax.random.split(jax.random.key(seed), 16)
    return {
        "dec_hidden": centred(keys[0], (QUERIES, CANDS, LENGTH, D), 1.0, 6.0, ((1, 2),)),
        "enc_keys": draw_enc_keys(jax.random.fold_in(keys[15], 71), 0),
        "enc_values": centred(keys[2], (QUERIES, SRC, D), 12.0, 72.0, ((1, 16),)),
        "enc_lengths": draw_enc_lengths(jax.random.fold_in(keys[15], 71), 0),
        "cand_counts": draw_cand_counts(jax.random.fold_in(keys[15], 71), 0),
        "gold_ids": set_ends(ranked(keys[5], (QUERIES, CANDS, LENGTH), VOCAB, 2), jax.random.fold_in(keys[5], 3), 0, VOCAB - 1).astype(jnp.int32),
        "gain_cross": jnp.clip(1.0 + 0.15 * jax.random.normal(keys[6], (D,), jnp.float32), 0.25, 1.75),
        "w_query": centred(keys[7], (D, D), D ** -0.5, 0.125, ((0, 2), (1, 16))),
        "w_out": centred(keys[8], (D, D), D ** -0.5, 0.125, ((0, 16), (1, 2))),
        "gain_ffn": jnp.clip(1.0 + 0.15 * jax.random.normal(keys[9], (D,), jnp.float32), 0.25, 1.75),
        "w_in_gate": centred(keys[10], (D, FF), D ** -0.5, 0.125, ((0, 2), (1, 16))),
        "w_in_up": centred(keys[11], (D, FF), D ** -0.5, 0.125, ((0, 2), (1, 16))),
        "w_ffn_out": centred(keys[12], (FF, D), (FF // 9) ** -0.5, 0.25, ((0, 16), (1, 2))),
        "gain_final": jnp.clip(1.0 + 0.15 * jax.random.normal(keys[13], (D,), jnp.float32), 0.25, 1.75),
        "w_vocab": draw_w_vocab(jax.random.fold_in(keys[15], 71), 0),
    }


norm_eps = 0.25

def root_norm(values, gain):
    squares = lax.optimization_barrier(jnp.mean(values * values, axis=-1, keepdims=True))
    return values * lax.rsqrt(squares + norm_eps) * gain

def reference(dec_hidden, enc_keys, enc_values, enc_lengths, cand_counts, gold_ids, gain_cross, w_query, w_out, gain_ffn, w_in_gate, w_in_up, w_ffn_out, gain_final, w_vocab):
    total_rows = QUERIES * CANDS * LENGTH
    inputs_flat = dec_hidden.reshape(total_rows, D).astype(jnp.float32)
    normed = root_norm(inputs_flat, gain_cross).astype(jnp.bfloat16)
    queries_all = jnp.dot(normed, w_query, preferred_element_type=jnp.float32).astype(jnp.bfloat16)
    queries_all = lax.optimization_barrier(queries_all)
    query_heads = queries_all.reshape(QUERIES, CANDS * LENGTH, HEADS, HEAD_DIM).transpose(2, 0, 1, 3).astype(jnp.float32)
    key_heads = enc_keys.reshape(QUERIES, SRC, HEADS, HEAD_DIM).transpose(2, 0, 1, 3).astype(jnp.float32)
    value_heads = enc_values.reshape(QUERIES, SRC, HEADS, HEAD_DIM).transpose(2, 0, 1, 3).astype(jnp.float32)
    live_keys = jnp.arange(SRC, dtype=jnp.int32)[None, :] < enc_lengths[:, None]

    def attend(operands):
        query_head, key_head, value_head = operands
        scores = jnp.einsum('brd,bsd->brs', query_head, key_head, precision=lax.Precision.HIGHEST)
        scores = jnp.where(live_keys[:, None, :], scores, -1e+30)
        row_max = lax.optimization_barrier(jnp.max(scores, axis=-1, keepdims=True))
        weights = jnp.where(live_keys[:, None, :], jnp.exp(scores - row_max), 0.0)
        denominator = lax.optimization_barrier(jnp.sum(weights, axis=-1, keepdims=True))
        rounded = lax.optimization_barrier(weights.astype(jnp.bfloat16)).astype(jnp.float32)
        mixed_values = jnp.einsum('brs,bsd->brd', rounded, value_head, precision=lax.Precision.HIGHEST)
        return (mixed_values / denominator).astype(jnp.bfloat16)
    attended = lax.map(attend, (query_heads, key_heads, value_heads))
    attended = attended.transpose(1, 2, 0, 3).reshape(total_rows, D)
    after_cross = inputs_flat + jnp.dot(attended, w_out, preferred_element_type=jnp.float32)
    normed_ffn = root_norm(after_cross, gain_ffn).astype(jnp.bfloat16)
    gate_part = jnp.dot(normed_ffn, w_in_gate, preferred_element_type=jnp.float32)
    up_part = jnp.dot(normed_ffn, w_in_up, preferred_element_type=jnp.float32)
    hidden = (jax.nn.gelu(gate_part, approximate=True) * up_part).astype(jnp.bfloat16)
    after_ffn = after_cross + jnp.dot(hidden, w_ffn_out, preferred_element_type=jnp.float32)
    normed_final = root_norm(after_ffn, gain_final).astype(jnp.bfloat16)
    block_rows = 512 if total_rows % 512 == 0 else total_rows

    def score_block(operands):
        rows_block, gold_block = operands
        logits = jnp.dot(rows_block, w_vocab, preferred_element_type=jnp.float32)
        row_max = lax.optimization_barrier(jnp.max(logits, axis=1))
        sum_exp = lax.optimization_barrier(jnp.sum(jnp.exp(logits - row_max[:, None]), axis=1))
        picked = jnp.take_along_axis(logits, gold_block[:, None], axis=1)[:, 0]
        return picked - row_max - jnp.log(sum_exp)
    logprob = lax.map(score_block, (normed_final.reshape(-1, block_rows, D), gold_ids.reshape(-1, block_rows)))
    per_cand = lax.optimization_barrier(jnp.mean(logprob.reshape(QUERIES, CANDS, LENGTH), axis=2))
    valid_cand = jnp.arange(CANDS, dtype=jnp.int32)[None, :] < cand_counts[:, None]
    cand_scores = jnp.where(valid_cand, per_cand, 0.0)
    best_score = lax.optimization_barrier(jnp.max(jnp.where(valid_cand, per_cand, -1e+30), axis=1))
    return (cand_scores, best_score)
```

```python
import functools

import jax
import jax.numpy as jnp
from jax import lax
from jax.experimental import pallas as pl
from jax.experimental.pallas import tpu as pltpu
from jax.sharding import PartitionSpec as P

HEAD_DIM = 64
NORM_EPS = 0.25
NEG = -1e30


VMEM = pltpu.VMEM
SMEM = pltpu.SMEM


def vmem_spec():
    return pl.BlockSpec(memory_space=VMEM)


def smem_spec():
    return pl.BlockSpec(memory_space=SMEM)


def any_spec():
    return pl.BlockSpec(memory_space=pl.ANY)


def dot32(a, b):
    return jnp.dot(a, b, preferred_element_type=jnp.float32)


def gelu_tanh(v):
    inner = 0.7978845608028654 * (v + 0.044715 * (v * v * v))
    return 0.5 * v * (1.0 + jnp.tanh(inner))


def attention_kernel(live_ref, mine_ref, peer_ref, kv_ref, out_ref):
    src = kv_ref.shape[0] * kv_ref.shape[2]
    cols = kv_ref.shape[3]
    keys = kv_ref[:, 0].reshape(src, cols)
    values = kv_ref[:, 1].reshape(src, cols)
    token = lax.broadcasted_iota(jnp.int32, (1, src), 1)
    bias = jnp.where(token < live_ref[0], 0.0, NEG).astype(jnp.float32)
    lane_head = lax.broadcasted_iota(jnp.int32, (1, cols), 1) // HEAD_DIM
    rows = mine_ref.shape[0]
    step = min(rows, 128)
    for part, q_ref in enumerate((mine_ref, peer_ref)):
        for start in range(0, rows, step):
            q = q_ref[start : start + step, :]
            mixed = jnp.zeros((step, cols), jnp.float32)
            for head in range(cols // HEAD_DIM):
                q_head = jnp.where(lane_head == head, q, jnp.zeros_like(q))
                scores = lax.dot_general(
                    q_head, keys, (((1,), (1,)), ((), ())), preferred_element_type=jnp.float32
                )
                scores = scores + bias
                row_max = jnp.max(scores, axis=-1, keepdims=True)
                weights = jnp.exp(scores - row_max)
                denominator = jnp.sum(weights, axis=-1, keepdims=True)
                head_out = dot32(weights.astype(jnp.bfloat16), values) / denominator
                mixed = jnp.where(lane_head == head, head_out, mixed)
            out_ref[part, start : start + step, :] = mixed.astype(jnp.bfloat16)


def attention(live, mine, peer, kv):
    rows, cols = mine.shape
    return pl.pallas_call(
        attention_kernel,
        out_shape=jax.ShapeDtypeStruct((2, rows, cols), jnp.bfloat16),
        in_specs=[smem_spec(), vmem_spec(), vmem_spec(), vmem_spec()],
        out_specs=vmem_spec(),
        name="attention",
    )(live, mine, peer, kv)


def project_kernel(n_cand, count, chip_ref, own_ref, par_ref, *refs):
    weights = refs[: 2 * n_cand]
    outs = refs[2 * n_cand : 2 * n_cand + count]
    own_s, par_s = refs[2 * n_cand + count :]
    share = own_ref.shape[0] // count
    for j in range(count):
        at = pl.multiple_of((chip_ref[0] ^ j) * share, share)
        own_s[j * share : (j + 1) * share, :] = own_ref[pl.ds(at, share), :]
        par_s[j * share : (j + 1) * share, :] = par_ref[pl.ds(at, share), :]
    own, par = own_s[...], par_s[...]
    width = weights[0].shape[1]
    for s in range(n_cand):
        block = dot32(own, weights[s][...]) + dot32(par, weights[n_cand + s][...])
        block = block.astype(jnp.bfloat16)
        for j in range(count):
            outs[j][:, s * width : (s + 1) * width] = block[j * share : (j + 1) * share, :]


def project(chip, own, par, weights, count):
    rows, cols = own.shape
    n_cand = len(weights) // 2
    model = weights[0].shape[1] * n_cand
    return pl.pallas_call(
        functools.partial(project_kernel, n_cand, count),
        out_shape=[jax.ShapeDtypeStruct((rows // count, model), jnp.bfloat16)] * count,
        in_specs=[smem_spec()] + [vmem_spec()] * (2 + len(weights)),
        out_specs=[vmem_spec()] * count,
        scratch_shapes=[VMEM((rows, cols), jnp.bfloat16)] * 2,
        name="project",
    )(chip, own, par, *weights)


def residual_kernel(count, base_ref, gain_ref, *refs):
    total = base_ref[...].astype(jnp.float32)
    for part in refs[:count]:
        total = total + part[...].astype(jnp.float32)
    squares = jnp.mean(total * total, axis=-1, keepdims=True)
    refs[count][...] = (total * lax.rsqrt(squares + NORM_EPS) * gain_ref[...]).astype(jnp.bfloat16)
    if len(refs) > count + 1:
        refs[count + 1][...] = total


def residual_norm(base, gain, parts, keep):
    shapes = [jax.ShapeDtypeStruct(base.shape, jnp.bfloat16)]
    if keep:
        shapes.append(jax.ShapeDtypeStruct(base.shape, jnp.float32))
    return pl.pallas_call(
        functools.partial(residual_kernel, len(parts)),
        out_shape=shapes,
        in_specs=[vmem_spec()] * (2 + len(parts)),
        out_specs=[vmem_spec()] * len(shapes),
        name="residual_norm",
    )(base, gain, *parts)


def ffn_kernel(n_cand, count, *refs):
    n_w = 2 * n_cand
    rows_in = refs[:count]
    gates = refs[count : count + n_w]
    ups = refs[count + n_w : count + 2 * n_w]
    downs = refs[count + 2 * n_w : count + 3 * n_w]
    outs = refs[count + 3 * n_w : 2 * count + 3 * n_w]
    scratch = refs[2 * count + 3 * n_w :]
    acts, gate_s, up_s, down_s, sems = scratch
    share = rows_in[0].shape[0]
    copies = []

    def fetch(source, target):
        copy = pltpu.make_async_copy(source, target, sems.at[len(copies)])
        copy.start()
        copies.append(copy)
        return copy

    row_copies = [fetch(rows_in[j], acts.at[pl.ds(j * share, share)]) for j in range(count)]
    gate_copies, up_copies, down_copies = [], [], []
    for i in range(n_w):
        gate_copies.append(fetch(gates[i], gate_s.at[i]))
        up_copies.append(fetch(ups[i], up_s.at[i]))
    for i in range(n_w):
        down_copies.append(fetch(downs[i], down_s.at[i]))
    for copy in row_copies:
        copy.wait()
    depth = gates[0].shape[0]
    hidden = []
    for side in range(2):
        gate_part, up_part = None, None
        for s in range(n_cand):
            i = side * n_cand + s
            block = acts[:, s * depth : (s + 1) * depth]
            gate_copies[i].wait()
            term = dot32(block, gate_s[i])
            gate_part = term if gate_part is None else gate_part + term
            up_copies[i].wait()
            term = dot32(block, up_s[i])
            up_part = term if up_part is None else up_part + term
        hidden.append((gelu_tanh(gate_part) * up_part).astype(jnp.bfloat16))
    width = downs[0].shape[1]
    for copy in down_copies:
        copy.wait()
    for s in range(n_cand):
        block = dot32(hidden[0], down_s[s]) + dot32(hidden[1], down_s[n_cand + s])
        block = block.astype(jnp.bfloat16)
        for j in range(count):
            outs[j][:, s * width : (s + 1) * width] = block[j * share : (j + 1) * share, :]


def feed_forward(rows_in, gates, ups, downs):
    count, n_w = len(rows_in), len(gates)
    n_cand = n_w // 2
    share, model = rows_in[0].shape
    return pl.pallas_call(
        functools.partial(ffn_kernel, n_cand, count),
        out_shape=[jax.ShapeDtypeStruct((share, model), jnp.bfloat16)] * count,
        in_specs=[any_spec()] * (count + 3 * n_w),
        out_specs=[vmem_spec()] * count,
        scratch_shapes=[
            VMEM((share * count, model), jnp.bfloat16),
            VMEM((n_w,) + gates[0].shape, jnp.bfloat16),
            VMEM((n_w,) + ups[0].shape, jnp.bfloat16),
            VMEM((n_w,) + downs[0].shape, jnp.bfloat16),
            pltpu.SemaphoreType.DMA((count + 3 * n_w,)),
        ],
        name="feed_forward",
    )(*rows_in, *gates, *ups, *downs)


def vocab_kernel(n_cand, count, vocab, start_ref, gold_ref, *refs):
    n_w = 2 * n_cand
    rows_in = refs[:count]
    weights = refs[count : count + n_w]
    out_ref, acts, max_s, sum_s, gold_s = refs[count + n_w :]
    step = pl.program_id(0)
    share = rows_in[0].shape[0]

    @pl.when(step == 0)
    def _():
        for j in range(count):
            acts[j * share : (j + 1) * share, :] = rows_in[j][...]
        max_s[...] = jnp.full_like(max_s, NEG)
        sum_s[...] = jnp.zeros_like(sum_s)
        gold_s[...] = jnp.zeros_like(gold_s)

    depth, width = weights[0].shape
    column = step * width + lax.broadcasted_iota(jnp.int32, (1, width), 1)
    for side in range(2):
        logits = None
        for s in range(n_cand):
            term = dot32(acts[:, s * depth : (s + 1) * depth], weights[side * n_cand + s][...])
            logits = term if logits is None else logits + term
        hit = column == gold_ref[...] - start_ref[side]
        inside = column < vocab
        gold_s[...] += jnp.sum(jnp.where(hit & inside, logits, 0.0), axis=1, keepdims=True)
        logits = jnp.where(inside, logits, NEG)
        old = max_s[...]
        new = jnp.maximum(old, jnp.max(logits, axis=1, keepdims=True))
        terms = jnp.sum(jnp.exp(logits - new), axis=1, keepdims=True)
        sum_s[...] = sum_s[...] * jnp.exp(old - new) + terms
        max_s[...] = new

    @pl.when(step == pl.num_programs(0) - 1)
    def _():
        lane = lax.broadcasted_iota(jnp.int32, out_ref.shape, 1)
        out_ref[...] = jnp.where(
            lane == 0, max_s[...], jnp.where(lane == 1, sum_s[...], gold_s[...])
        )


def vocab_scores(starts, gold, rows_in, weights):
    count, n_w = len(rows_in), len(weights)
    n_cand = n_w // 2
    share, model = rows_in[0].shape
    depth, vocab = weights[0].shape
    rows = share * count
    width = 256
    whole = pl.BlockSpec((share, model), lambda i: (0, 0))
    column = pl.BlockSpec((depth, width), lambda i: (0, i))
    return pl.pallas_call(
        functools.partial(vocab_kernel, n_cand, count, vocab),
        grid=(pl.cdiv(vocab, width),),
        out_shape=jax.ShapeDtypeStruct((rows, 128), jnp.float32),
        in_specs=[smem_spec(), pl.BlockSpec((rows, 1), lambda i: (0, 0))]
        + [whole] * count
        + [column] * n_w,
        out_specs=pl.BlockSpec((rows, 128), lambda i: (0, 0)),
        scratch_shapes=[VMEM((rows, model), jnp.bfloat16)] + [VMEM((rows, 1), jnp.float32)] * 3,
        name="vocab_scores",
    )(starts, gold, *rows_in, *weights)


def body(
    dec_hidden,
    enc_keys,
    enc_values,
    enc_lengths,
    cand_counts,
    gold_ids,
    gain_cross,
    w_query,
    w_out,
    gain_ffn,
    w_in_gate,
    w_in_up,
    w_ffn_out,
    gain_final,
    w_vocab,
):
    queries, cand_dev, length, model = dec_hidden.shape
    n_tok, n_cand = lax.axis_size("tok"), lax.axis_size("cand")
    tok, cand = lax.axis_index("tok"), lax.axis_index("cand")
    core, chip = tok % 2, tok // 2
    chips = n_tok // 2
    rows = cand_dev * length
    share = rows // chips
    block = model // n_cand
    head_cols = w_query.shape[1]
    half = n_cand // 2
    assert queries == 2 and n_cand % 2 == 0 and n_tok % 4 == 0 and n_tok & (n_tok - 1) == 0

    def swap(a, k):
        return lax.ppermute(a, "tok", [(i, i ^ k) for i in range(n_tok)])

    def from_cands(a):
        return [a] + [
            lax.ppermute(a, "cand", [(i, (i - s) % n_cand) for i in range(n_cand)])
            for s in range(1, n_cand)
        ]

    def with_partner(parts):
        return parts + [swap(a, 1) for a in parts]

    def rolled(a):
        return jnp.concatenate(
            [
                lax.dynamic_slice_in_dim(a, ((cand + s) % n_cand) * block, block, a.ndim - 1)
                for s in range(n_cand)
            ],
            axis=-1,
        )

    def gather_rows(a):
        out = [None] * chips
        out[0] = a
        for j in range(2, chips, 2):
            out[j] = swap(a, 2 * j)
        for j in range(0, chips, 2):
            out[j + 1] = swap(out[j], 2)
        return out

    def scatter_rows(parts):
        return [parts[0]] + [swap(parts[j], 2 * j) for j in range(1, chips)]

    query_at = cand // half

    pair = jnp.stack(
        [
            lax.dynamic_index_in_dim(enc_keys, query_at, 0, keepdims=False),
            lax.dynamic_index_in_dim(enc_values, query_at, 0, keepdims=False),
        ]
    )
    pair = pair.reshape(2, pair.shape[1], n_tok, head_cols).transpose(2, 0, 1, 3)
    key_values = lax.all_to_all(pair, "tok", 0, 0, tiled=True)

    query_parts = from_cands(w_query)
    out_parts = with_partner(from_cands(w_out))
    gate_parts = with_partner(from_cands(w_in_gate))
    up_parts = with_partner(from_cands(w_in_up))

    flat = rolled(dec_hidden.reshape(queries * rows, model))
    wide = flat.astype(jnp.float32)
    gain_first, gain_mid, gain_last = (
        rolled(g.reshape(1, model)) for g in (gain_cross, gain_ffn, gain_final)
    )
    squares = jnp.mean(wide * wide, axis=-1, keepdims=True)
    normed = (wide * lax.rsqrt(squares + NORM_EPS) * gain_first).astype(jnp.bfloat16)
    query = sum(
        dot32(normed[:, s * block : (s + 1) * block], query_parts[s]) for s in range(n_cand)
    ).astype(jnp.bfloat16)
    query = query.reshape(queries, rows, head_cols)
    mine = lax.dynamic_index_in_dim(query, query_at, 0, keepdims=False)
    other = lax.dynamic_index_in_dim(query, 1 - query_at, 0, keepdims=False)
    across = [(i, (i + half) % n_cand) for i in range(n_cand)]
    peer = lax.ppermute(other, "cand", across)
    live = lax.dynamic_slice_in_dim(enc_lengths, query_at, 1, 0)
    attended = attention(live, mine, peer, key_values)

    def route(flip):
        perm = []
        for t in range(n_tok):
            for c in range(n_cand):
                to_half = (t % 2) ^ flip
                to = (t - t % 2 + c // half) * n_cand + c % half + to_half * half
                perm.append((t * n_cand + c, to))
        return perm

    own_rows, peer_rows = attended[0], attended[1]
    straight = core == query_at
    first = lax.ppermute(jnp.where(straight, own_rows, peer_rows), ("tok", "cand"), route(0))
    second = lax.ppermute(jnp.where(straight, peer_rows, own_rows), ("tok", "cand"), route(1))
    att_own = jnp.where(straight, first, second)
    att_par = jnp.where(straight, second, first)
    chip_at = chip.reshape(1)
    cross_terms = scatter_rows(project(chip_at, att_own, att_par, out_parts, chips))

    late_down, late_vocab, _ = lax.optimization_barrier((w_ffn_out, w_vocab, att_own))
    down_parts = with_partner(from_cands(late_down))
    vocab_parts = with_partner(from_cands(late_vocab))

    base = lax.dynamic_slice_in_dim(flat, core * rows + chip * share, share, 0)
    normed_ffn, after_cross = residual_norm(base, gain_mid, cross_terms, True)
    ffn_terms = scatter_rows(
        feed_forward(gather_rows(normed_ffn), gate_parts, up_parts, down_parts)
    )
    (normed_final,) = residual_norm(after_cross, gain_last, ffn_terms, False)

    order = chip ^ jnp.arange(chips)
    gold = lax.dynamic_index_in_dim(gold_ids, core, 0, keepdims=False).reshape(chips, share)
    gold = gold[order].reshape(rows, 1)
    vocab_dev = w_vocab.shape[1]
    starts = jnp.stack([tok * vocab_dev, (tok ^ 1) * vocab_dev])
    stats = vocab_scores(starts, gold, gather_rows(normed_final), vocab_parts)
    stats = stats[:, :3].reshape(chips, share, 3)[order].reshape(rows, 3).T
    k = 2
    while k < n_tok:
        theirs = swap(stats, k)
        top = jnp.maximum(stats[0], theirs[0])
        total = stats[1] * jnp.exp(stats[0] - top) + theirs[1] * jnp.exp(theirs[0] - top)
        stats = jnp.stack([top, total, stats[2] + theirs[2]])
        k *= 2
    logprob = stats[2] - stats[0] - jnp.log(stats[1])
    per_cand = jnp.mean(logprob.reshape(cand_dev, length), axis=1)
    both = jnp.stack([per_cand, swap(per_cand, 1)])
    both = jnp.where(core == 0, both, both[::-1])
    cand_index = cand * cand_dev + lax.iota(jnp.int32, cand_dev)
    valid = cand_index[None, :] < cand_counts[:, None]
    cand_scores = jnp.where(valid, both, 0.0)
    best = jnp.max(jnp.where(valid, both, NEG), axis=1)
    k = 1
    while k < n_cand:
        best = jnp.maximum(
            best, lax.ppermute(best, "cand", [(i, i ^ k) for i in range(n_cand)])
        )
        k *= 2
    return (cand_scores, best)


def solution(mesh):
    in_specs = (
        P(None, "cand", None, None),
        P(None, "tok", None),
        P(None, "tok", None),
        P(),
        P(),
        P(None, "cand", None),
        P(),
        P("cand", "tok"),
        P("tok", "cand"),
        P(),
        P("cand", "tok"),
        P("cand", "tok"),
        P("tok", "cand"),
        P(),
        P("cand", "tok"),
    )
    out_specs = (P(None, "cand"), P())
    return jax.shard_map(body, mesh=mesh, in_specs=in_specs, out_specs=out_specs, check_vma=False)
```

```python
import functools

import jax
import jax.numpy as jnp
from jax import lax
from jax.experimental import pallas as pl
from jax.experimental.pallas import tpu as pltpu
from jax.sharding import PartitionSpec as P


HEAD_DIM = 64
NORM_EPS = 0.25
NEG = -1e30
VOCAB_STEP = 256


VMEM = pltpu.VMEM
SMEM = pltpu.SMEM


def vmem_spec():
    return pl.BlockSpec(memory_space=VMEM)


def smem_spec():
    return pl.BlockSpec(memory_space=SMEM)


def any_spec():
    return pl.BlockSpec(memory_space=pl.ANY)


def dot32(a, b):
    return jnp.dot(a, b, preferred_element_type=jnp.float32)


def dot32_t(a, b):
    return lax.dot_general(a, b, (((1,), (1,)), ((), ())), preferred_element_type=jnp.float32)


def gelu_tanh(v):
    inner = 0.7978845608028654 * (v + 0.044715 * (v * v * v))
    return 0.5 * v * (1.0 + jnp.tanh(inner))


def attention_kernel(live_ref, mine_ref, peer_ref, kv_ref, out_ref):
    src = kv_ref.shape[0] * kv_ref.shape[2]
    cols = kv_ref.shape[3]
    keys = kv_ref[:, 0].reshape(src, cols)
    values = kv_ref[:, 1].reshape(src, cols)
    token = lax.broadcasted_iota(jnp.int32, (1, src), 1)
    bias = jnp.where(token < live_ref[0], 0.0, NEG).astype(jnp.float32)
    lane_head = lax.broadcasted_iota(jnp.int32, (1, cols), 1) // HEAD_DIM
    rows = mine_ref.shape[0]
    step = min(rows, 128)
    for part, q_ref in enumerate((mine_ref, peer_ref)):
        for start in range(0, rows, step):
            q = q_ref[start : start + step, :]
            mixed = jnp.zeros((step, cols), jnp.float32)
            for head in range(cols // HEAD_DIM):
                q_head = jnp.where(lane_head == head, q, jnp.zeros_like(q))
                scores = dot32_t(q_head, keys) + bias
                row_max = jnp.max(scores, axis=-1, keepdims=True)
                weights = jnp.exp(scores - row_max)
                denominator = jnp.sum(weights, axis=-1, keepdims=True)
                head_out = dot32(weights.astype(jnp.bfloat16), values) / denominator
                mixed = jnp.where(lane_head == head, head_out, mixed)
            out_ref[part, start : start + step, :] = mixed.astype(jnp.bfloat16)


def attention(live, mine, peer, kv):
    rows, cols = mine.shape
    return pl.pallas_call(
        attention_kernel,
        out_shape=jax.ShapeDtypeStruct((2, rows, cols), jnp.bfloat16),
        in_specs=[smem_spec(), vmem_spec(), vmem_spec(), vmem_spec()],
        out_specs=vmem_spec(),
        name="attention",
    )(live, mine, peer, kv)


def project_kernel(n_cand, count, chip_ref, own_ref, par_ref, *refs):
    weights = refs[: 2 * n_cand]
    outs = refs[2 * n_cand : 2 * n_cand + count]
    own_s, par_s = refs[2 * n_cand + count :]
    share = own_ref.shape[0] // count
    for j in range(count):
        at = pl.multiple_of((chip_ref[0] ^ j) * share, share)
        own_s[j * share : (j + 1) * share, :] = own_ref[pl.ds(at, share), :]
        par_s[j * share : (j + 1) * share, :] = par_ref[pl.ds(at, share), :]
    own, par = own_s[...], par_s[...]
    width = weights[0].shape[1]
    for s in range(n_cand):
        block = dot32(own, weights[s][...]) + dot32(par, weights[n_cand + s][...])
        block = block.astype(jnp.bfloat16)
        for j in range(count):
            outs[j][:, s * width : (s + 1) * width] = block[j * share : (j + 1) * share, :]


def project(chip, own, par, weights, count):
    rows, cols = own.shape
    n_cand = len(weights) // 2
    model = weights[0].shape[1] * n_cand
    return pl.pallas_call(
        functools.partial(project_kernel, n_cand, count),
        out_shape=[jax.ShapeDtypeStruct((rows // count, model), jnp.bfloat16)] * count,
        in_specs=[smem_spec()] + [vmem_spec()] * (2 + len(weights)),
        out_specs=[vmem_spec()] * count,
        scratch_shapes=[VMEM((rows, cols), jnp.bfloat16)] * 2,
        name="project",
    )(chip, own, par, *weights)


def residual_kernel(count, base_ref, gain_ref, *refs):
    total = base_ref[...].astype(jnp.float32)
    for part in refs[:count]:
        total = total + part[...].astype(jnp.float32)
    squares = jnp.mean(total * total, axis=-1, keepdims=True)
    refs[count][...] = (total * lax.rsqrt(squares + NORM_EPS) * gain_ref[...]).astype(jnp.bfloat16)
    if len(refs) > count + 1:
        refs[count + 1][...] = total


def residual_norm(base, gain, parts, keep):
    shapes = [jax.ShapeDtypeStruct(base.shape, jnp.bfloat16)]
    if keep:
        shapes.append(jax.ShapeDtypeStruct(base.shape, jnp.float32))
    return pl.pallas_call(
        functools.partial(residual_kernel, len(parts)),
        out_shape=shapes,
        in_specs=[vmem_spec()] * (2 + len(parts)),
        out_specs=[vmem_spec()] * len(shapes),
        name="residual_norm",
    )(base, gain, *parts)


def ffn_kernel(n_cand, count, *refs):
    n_w = 2 * n_cand
    rows_in = refs[:count]
    gates = refs[count : count + n_w]
    ups = refs[count + n_w : count + 2 * n_w]
    downs = refs[count + 2 * n_w : count + 3 * n_w]
    outs = refs[count + 3 * n_w : 2 * count + 3 * n_w]
    scratch = refs[2 * count + 3 * n_w :]
    acts, gate_s, up_s, down_s, sems = scratch
    share = rows_in[0].shape[0]
    copies = []

    def fetch(source, target):
        copy = pltpu.make_async_copy(source, target, sems.at[len(copies)])
        copy.start()
        copies.append(copy)
        return copy

    row_copies = [fetch(rows_in[j], acts.at[pl.ds(j * share, share)]) for j in range(count)]
    gate_copies, up_copies, down_copies = [], [], []
    for i in range(n_w):
        gate_copies.append(fetch(gates[i], gate_s.at[i]))
        up_copies.append(fetch(ups[i], up_s.at[i]))
    for i in range(n_w):
        down_copies.append(fetch(downs[i], down_s.at[i]))
    for copy in row_copies:
        copy.wait()
    depth = gates[0].shape[1]
    hidden = []
    for side in range(2):
        gate_part, up_part = None, None
        for s in range(n_cand):
            i = side * n_cand + s
            block = acts[:, s * depth : (s + 1) * depth]
            gate_copies[i].wait()
            term = dot32_t(block, gate_s[i])
            gate_part = term if gate_part is None else gate_part + term
            up_copies[i].wait()
            term = dot32_t(block, up_s[i])
            up_part = term if up_part is None else up_part + term
        hidden.append((gelu_tanh(gate_part) * up_part).astype(jnp.bfloat16))
    width = downs[0].shape[1]
    for copy in down_copies:
        copy.wait()
    for s in range(n_cand):
        block = dot32(hidden[0], down_s[s]) + dot32(hidden[1], down_s[n_cand + s])
        block = block.astype(jnp.bfloat16)
        for j in range(count):
            outs[j][:, s * width : (s + 1) * width] = block[j * share : (j + 1) * share, :]


def feed_forward(rows_in, gates, ups, downs):
    count, n_w = len(rows_in), len(gates)
    n_cand = n_w // 2
    share, model = rows_in[0].shape
    return pl.pallas_call(
        functools.partial(ffn_kernel, n_cand, count),
        out_shape=[jax.ShapeDtypeStruct((share, model), jnp.bfloat16)] * count,
        in_specs=[any_spec()] * (count + 3 * n_w),
        out_specs=[vmem_spec()] * count,
        scratch_shapes=[
            VMEM((share * count, model), jnp.bfloat16),
            VMEM((n_w,) + gates[0].shape, jnp.bfloat16),
            VMEM((n_w,) + ups[0].shape, jnp.bfloat16),
            VMEM((n_w,) + downs[0].shape, jnp.bfloat16),
            pltpu.SemaphoreType.DMA((count + 3 * n_w,)),
        ],
        name="feed_forward",
    )(*rows_in, *gates, *ups, *downs)


def vocab_kernel(n_cand, count, n_src, first, end, start_ref, gold_ref, *refs):
    n_w = 2 * n_cand
    rows_in = refs[:count]
    weights = refs[count : count + n_w]
    carried = refs[count + n_w : count + n_w + n_src]
    out_ref, acts = refs[count + n_w + n_src :]
    step = pl.program_id(0)
    share = rows_in[0].shape[0]
    rows = share * count

    @pl.when(step == 0)
    def _():
        for j in range(count):
            acts[j * share : (j + 1) * share, :] = rows_in[j][...]
        if n_src:
            out_ref[...] = carried[0][...]
        else:
            out_ref[0] = jnp.full((8, rows), NEG, jnp.float32)
            out_ref[1] = jnp.zeros((8, rows), jnp.float32)
            out_ref[2] = jnp.zeros((8, rows), jnp.float32)

    width, depth = weights[0].shape
    column = (first + step) * width + lax.broadcasted_iota(jnp.int32, (width, 1), 0)
    inside = column < end
    for side in range(2):
        logits = None
        for s in range(n_cand):
            term = dot32_t(weights[side * n_cand + s][...], acts[:, s * depth : (s + 1) * depth])
            logits = term if logits is None else logits + term
        hit = (column == gold_ref[...] - start_ref[side]) & inside
        picked = jnp.where(hit, logits, 0.0).reshape(width // 8, 8, rows)
        out_ref[2] += jnp.sum(picked, axis=0)
        logits = jnp.where(inside, logits, NEG).reshape(width // 8, 8, rows)
        old = out_ref[0]
        new = jnp.maximum(old, jnp.max(logits, axis=0))
        terms = jnp.sum(jnp.exp(logits - new[None]), axis=0)
        out_ref[1] = out_ref[1] * jnp.exp(old - new) + terms
        out_ref[0] = new


def vocab_scores(starts, gold, rows_in, weights, whole, begin, end, carried):
    count, n_w = len(rows_in), len(weights)
    n_cand = n_w // 2
    share, model = rows_in[0].shape
    depth = weights[0].shape[1]
    rows = share * count
    width = VOCAB_STEP
    first = begin // width
    constant = pl.BlockSpec((share, model), lambda i: (0, 0))
    stats = pl.BlockSpec((3, 8, rows), lambda i: (0, 0, 0))
    columns = [
        pl.BlockSpec((width, depth), lambda i: (first + i, 0))
        if is_whole
        else pl.BlockSpec((width, depth), lambda i: (i, 0))
        for is_whole in whole
    ]
    return pl.pallas_call(
        functools.partial(vocab_kernel, n_cand, count, len(carried), first, end),
        grid=(pl.cdiv(end - begin, width),),
        out_shape=jax.ShapeDtypeStruct((3, 8, rows), jnp.float32),
        in_specs=[smem_spec(), pl.BlockSpec((1, rows), lambda i: (0, 0))]
        + [constant] * count
        + columns
        + [stats] * len(carried),
        out_specs=stats,
        scratch_shapes=[VMEM((rows, model), jnp.bfloat16)],
        name="vocab_scores",
    )(starts, gold, *rows_in, *weights, *carried)


def body(
    dec_hidden,
    enc_keys,
    enc_values,
    enc_lengths,
    cand_counts,
    gold_ids,
    gain_cross,
    w_query,
    w_out,
    gain_ffn,
    w_in_gate,
    w_in_up,
    w_ffn_out,
    gain_final,
    w_vocab,
):
    queries, cand_dev, length, model = dec_hidden.shape
    n_tok, n_cand = lax.axis_size("tok"), lax.axis_size("cand")
    tok, cand = lax.axis_index("tok"), lax.axis_index("cand")
    core, chip = tok % 2, tok // 2
    chips = n_tok // 2
    rows = cand_dev * length
    share = rows // chips
    block = model // n_cand
    head_cols = w_query.shape[1]
    half = n_cand // 2
    assert queries == 2 and n_cand % 2 == 0 and n_tok % 4 == 0 and n_tok & (n_tok - 1) == 0

    def swap(a, k):
        return lax.ppermute(a, "tok", [(i, i ^ k) for i in range(n_tok)])

    def across(a, shift):
        return lax.ppermute(a, "cand", [(i, (i - shift) % n_cand) for i in range(n_cand)])

    def from_cands(a):
        return [a] + [across(a, s) for s in range(1, n_cand)]

    def with_partner(parts):
        own = swap(parts[0], 1)
        return parts + [own] + [swap(a, 1) for a in parts[1:]]

    def rolled(a):
        return jnp.concatenate(
            [
                lax.dynamic_slice_in_dim(a, ((cand + s) % n_cand) * block, block, a.ndim - 1)
                for s in range(n_cand)
            ],
            axis=-1,
        )

    def gather_rows(a):
        out = [None] * chips
        out[0] = a
        for j in range(2, chips, 2):
            out[j] = swap(a, 2 * j)
        for j in range(0, chips, 2):
            out[j + 1] = swap(out[j], 2)
        return out

    def scatter_rows(parts):
        return [parts[0]] + [swap(parts[j], 2 * j) for j in range(1, chips)]

    query_at = cand // half

    pair = jnp.stack(
        [
            lax.dynamic_index_in_dim(enc_keys, query_at, 0, keepdims=False),
            lax.dynamic_index_in_dim(enc_values, query_at, 0, keepdims=False),
        ]
    )
    pair = pair.reshape(2, pair.shape[1], n_tok, head_cols).transpose(2, 0, 1, 3)
    key_values = lax.all_to_all(pair, "tok", 0, 0, tiled=True)

    query_parts = from_cands(w_query)
    out_parts = with_partner(from_cands(w_out))
    gate_parts = with_partner(from_cands(w_in_gate.T))
    up_parts = with_partner(from_cands(w_in_up.T))
    down_parts = with_partner(from_cands(w_ffn_out))
    vocab_all = w_vocab.T
    vocab_dev = vocab_all.shape[0]
    cut = pl.cdiv(vocab_dev, VOCAB_STEP) // 2 * VOCAB_STEP
    vocab_low = from_cands(vocab_all[:cut])[1:]
    vocab_high = from_cands(vocab_all[cut:])[1:]
    vocab_other = swap(vocab_all, 1)
    low = [vocab_all] + vocab_low + [vocab_other] + [swap(w, 1) for w in vocab_low]
    high = [vocab_all] + vocab_high + [vocab_other] + [swap(w, 1) for w in vocab_high]

    flat = rolled(dec_hidden.reshape(queries * rows, model))
    wide = flat.astype(jnp.float32)
    gain_first, gain_mid, gain_last = (
        rolled(g.reshape(1, model)) for g in (gain_cross, gain_ffn, gain_final)
    )
    squares = jnp.mean(wide * wide, axis=-1, keepdims=True)
    normed = (wide * lax.rsqrt(squares + NORM_EPS) * gain_first).astype(jnp.bfloat16)
    query = sum(
        dot32(normed[:, s * block : (s + 1) * block], query_parts[s]) for s in range(n_cand)
    ).astype(jnp.bfloat16)
    query = query.reshape(queries, rows, head_cols)
    mine = lax.dynamic_index_in_dim(query, query_at, 0, keepdims=False)
    other = lax.dynamic_index_in_dim(query, 1 - query_at, 0, keepdims=False)
    peer = across(other, half)
    live = lax.dynamic_slice_in_dim(enc_lengths, query_at, 1, 0)
    attended = attention(live, mine, peer, key_values)

    def route(a, flip):
        perm = []
        for t in range(n_tok):
            for c in range(n_cand):
                to_half = (t % 2) ^ flip
                to = (t - t % 2 + c // half) * n_cand + c % half + to_half * half
                perm.append((t * n_cand + c, to))
        return lax.ppermute(a, ("tok", "cand"), perm)

    own_rows, peer_rows = attended[0], attended[1]
    straight = core == query_at
    first = route(jnp.where(straight, own_rows, peer_rows), 0)
    second = route(jnp.where(straight, peer_rows, own_rows), 1)
    att_own = jnp.where(straight, first, second)
    att_par = jnp.where(straight, second, first)
    chip_at = chip.reshape(1)
    cross_terms = project(chip_at, att_own, att_par, out_parts, chips)
    cross_terms = scatter_rows(cross_terms)
    base = lax.dynamic_slice_in_dim(flat, core * rows + chip * share, share, 0)
    normed_ffn, after_cross = residual_norm(base, gain_mid, cross_terms, True)
    ffn_rows = gather_rows(normed_ffn)
    ffn_terms = feed_forward(ffn_rows, gate_parts, up_parts, down_parts)
    ffn_terms = scatter_rows(ffn_terms)
    (normed_final,) = residual_norm(after_cross, gain_last, ffn_terms, False)
    final_rows = gather_rows(normed_final)

    order = chip ^ jnp.arange(chips)
    gold = lax.dynamic_index_in_dim(gold_ids, core, 0, keepdims=False).reshape(chips, share)
    gold = gold[order].reshape(1, rows)
    starts = jnp.stack([tok * vocab_dev, (tok ^ 1) * vocab_dev])
    whole = ([True] + [False] * (n_cand - 1)) * 2
    stats = vocab_scores(starts, gold, final_rows, low, whole, 0, cut, [])
    stats = vocab_scores(starts, gold, final_rows, high, whole, cut, vocab_dev, [stats])
    top = jnp.max(stats[0], axis=0)
    stats = jnp.stack(
        [top, jnp.sum(stats[1] * jnp.exp(stats[0] - top), axis=0), jnp.sum(stats[2], axis=0)]
    )
    stats = stats.reshape(3, chips, share)[:, order].reshape(3, rows)
    k = 2
    while k < n_tok:
        theirs = swap(stats, k)
        top = jnp.maximum(stats[0], theirs[0])
        total = stats[1] * jnp.exp(stats[0] - top) + theirs[1] * jnp.exp(theirs[0] - top)
        stats = jnp.stack([top, total, stats[2] + theirs[2]])
        k *= 2
    logprob = stats[2] - stats[0] - jnp.log(stats[1])
    per_cand = jnp.mean(logprob.reshape(cand_dev, length), axis=1)
    both = jnp.stack([per_cand, swap(per_cand, 1)])
    both = jnp.where(core == 0, both, both[::-1])
    cand_index = cand * cand_dev + lax.iota(jnp.int32, cand_dev)
    valid = cand_index[None, :] < cand_counts[:, None]
    cand_scores = jnp.where(valid, both, 0.0)
    best = jnp.max(jnp.where(valid, both, NEG), axis=1)
    k = 1
    while k < n_cand:
        best = jnp.maximum(
            best, lax.ppermute(best, "cand", [(i, i ^ k) for i in range(n_cand)])
        )
        k *= 2
    return (cand_scores, best)


def solution(mesh):
    in_specs = (
        P(None, "cand", None, None),
        P(None, "tok", None),
        P(None, "tok", None),
        P(),
        P(),
        P(None, "cand", None),
        P(),
        P("cand", "tok"),
        P("tok", "cand"),
        P(),
        P("cand", "tok"),
        P("cand", "tok"),
        P("tok", "cand"),
        P(),
        P("cand", "tok"),
    )
    out_specs = (P(None, "cand"), P())
    return jax.shard_map(body, mesh=mesh, in_specs=in_specs, out_specs=out_specs, check_vma=False)
```

```python
import functools

import jax
import jax.numpy as jnp
from jax import lax
from jax.experimental import pallas as pl
from jax.experimental.pallas import tpu as pltpu
from jax.sharding import PartitionSpec as P


HEAD_DIM = 64
NORM_EPS = 0.25
NEG = -1e30
VOCAB_STEP = 256


VMEM = pltpu.VMEM
SMEM = pltpu.SMEM


def vmem_spec():
    return pl.BlockSpec(memory_space=VMEM)


def smem_spec():
    return pl.BlockSpec(memory_space=SMEM)


def any_spec():
    return pl.BlockSpec(memory_space=pl.ANY)


def dot32(a, b):
    return jnp.dot(a, b, preferred_element_type=jnp.float32)


def dot32_t(a, b):
    return lax.dot_general(a, b, (((1,), (1,)), ((), ())), preferred_element_type=jnp.float32)


def gelu_tanh(v):
    inner = 0.7978845608028654 * (v + 0.044715 * (v * v * v))
    return 0.5 * v * (1.0 + jnp.tanh(inner))


def attention_kernel(live_ref, mine_ref, peer_ref, kv_ref, first_ref, second_ref):
    src = kv_ref.shape[0] * kv_ref.shape[2]
    cols = kv_ref.shape[3]
    keys = kv_ref[:, 0].reshape(src, cols)
    values = kv_ref[:, 1].reshape(src, cols)
    token = lax.broadcasted_iota(jnp.int32, (1, src), 1)
    bias = jnp.where(token < live_ref[0], 0.0, NEG).astype(jnp.float32)
    lane_head = lax.broadcasted_iota(jnp.int32, (1, cols), 1) // HEAD_DIM
    rows = mine_ref.shape[0]
    step = min(rows, 128)
    straight = live_ref[1] == 1
    for out_ref, one_ref, two_ref in (
        (first_ref, mine_ref, peer_ref),
        (second_ref, peer_ref, mine_ref),
    ):
        for start in range(0, rows, step):
            at = slice(start, start + step)
            q = jnp.where(straight, one_ref[at, :], two_ref[at, :])
            mixed = jnp.zeros((step, cols), jnp.float32)
            for head in range(cols // HEAD_DIM):
                q_head = jnp.where(lane_head == head, q, jnp.zeros_like(q))
                scores = dot32_t(q_head, keys) + bias
                row_max = jnp.max(scores, axis=-1, keepdims=True)
                weights = jnp.exp(scores - row_max)
                denominator = jnp.sum(weights, axis=-1, keepdims=True)
                head_out = dot32(weights.astype(jnp.bfloat16), values) / denominator
                mixed = jnp.where(lane_head == head, head_out, mixed)
            out_ref[at, :] = mixed.astype(jnp.bfloat16)


def attention(live, mine, peer, kv):
    rows, cols = mine.shape
    return pl.pallas_call(
        attention_kernel,
        out_shape=[jax.ShapeDtypeStruct((rows, cols), jnp.bfloat16)] * 2,
        in_specs=[smem_spec(), vmem_spec(), vmem_spec(), vmem_spec()],
        out_specs=[vmem_spec()] * 2,
        name="attention",
    )(live, mine, peer, kv)


def project_kernel(n_cand, count, chip_ref, first_ref, second_ref, *refs):
    weights = refs[: 2 * n_cand]
    outs = refs[2 * n_cand : 2 * n_cand + count]
    own_s, par_s = refs[2 * n_cand + count :]
    share = first_ref.shape[0] // count
    straight = chip_ref[1] == 1
    for j in range(count):
        at = pl.multiple_of((chip_ref[0] ^ j) * share, share)
        to = slice(j * share, (j + 1) * share)
        first, second = first_ref[pl.ds(at, share), :], second_ref[pl.ds(at, share), :]
        own_s[to, :] = jnp.where(straight, first, second)
        par_s[to, :] = jnp.where(straight, second, first)
    own, par = own_s[...], par_s[...]
    width = weights[0].shape[1]
    for s in range(n_cand):
        block = dot32(own, weights[s][...]) + dot32(par, weights[n_cand + s][...])
        block = block.astype(jnp.bfloat16)
        for j in range(count):
            outs[j][:, s * width : (s + 1) * width] = block[j * share : (j + 1) * share, :]


def project(chip, first, second, weights, count):
    rows, cols = first.shape
    n_cand = len(weights) // 2
    model = weights[0].shape[1] * n_cand
    return pl.pallas_call(
        functools.partial(project_kernel, n_cand, count),
        out_shape=[jax.ShapeDtypeStruct((rows // count, model), jnp.bfloat16)] * count,
        in_specs=[smem_spec()] + [vmem_spec()] * (2 + len(weights)),
        out_specs=[vmem_spec()] * count,
        scratch_shapes=[VMEM((rows, cols), jnp.bfloat16)] * 2,
        name="project",
    )(chip, first, second, *weights)


def residual_kernel(count, base_ref, gain_ref, *refs):
    total = base_ref[...].astype(jnp.float32)
    for part in refs[:count]:
        total = total + part[...].astype(jnp.float32)
    squares = jnp.mean(total * total, axis=-1, keepdims=True)
    refs[count][...] = (total * lax.rsqrt(squares + NORM_EPS) * gain_ref[...]).astype(jnp.bfloat16)
    if len(refs) > count + 1:
        refs[count + 1][...] = total


def residual_norm(base, gain, parts, keep):
    shapes = [jax.ShapeDtypeStruct(base.shape, jnp.bfloat16)]
    if keep:
        shapes.append(jax.ShapeDtypeStruct(base.shape, jnp.float32))
    return pl.pallas_call(
        functools.partial(residual_kernel, len(parts)),
        out_shape=shapes,
        in_specs=[vmem_spec()] * (2 + len(parts)),
        out_specs=[vmem_spec()] * len(shapes),
        name="residual_norm",
    )(base, gain, *parts)


def ffn_kernel(n_cand, count, *refs):
    n_w = 2 * n_cand
    rows_in = refs[:count]
    gates = refs[count : count + n_w]
    ups = refs[count + n_w : count + 2 * n_w]
    downs = refs[count + 2 * n_w : count + 3 * n_w]
    outs = refs[count + 3 * n_w : 2 * count + 3 * n_w]
    scratch = refs[2 * count + 3 * n_w :]
    acts, gate_s, up_s, down_s, sems = scratch
    share = rows_in[0].shape[0]
    copies = []

    def fetch(source, target):
        copy = pltpu.make_async_copy(source, target, sems.at[len(copies)])
        copy.start()
        copies.append(copy)
        return copy

    row_copies = [fetch(rows_in[j], acts.at[pl.ds(j * share, share)]) for j in range(count)]
    gate_copies, up_copies, down_copies = [], [], []
    for i in range(n_w):
        gate_copies.append(fetch(gates[i], gate_s.at[i]))
        up_copies.append(fetch(ups[i], up_s.at[i]))
    for i in range(n_w):
        down_copies.append(fetch(downs[i], down_s.at[i]))
    for copy in row_copies:
        copy.wait()
    depth = gates[0].shape[1]
    hidden = []
    for side in range(2):
        gate_part, up_part = None, None
        for s in range(n_cand):
            i = side * n_cand + s
            block = acts[:, s * depth : (s + 1) * depth]
            gate_copies[i].wait()
            term = dot32_t(block, gate_s[i])
            gate_part = term if gate_part is None else gate_part + term
            up_copies[i].wait()
            term = dot32_t(block, up_s[i])
            up_part = term if up_part is None else up_part + term
        hidden.append((gelu_tanh(gate_part) * up_part).astype(jnp.bfloat16))
    width = downs[0].shape[1]
    for copy in down_copies:
        copy.wait()
    for s in range(n_cand):
        block = dot32(hidden[0], down_s[s]) + dot32(hidden[1], down_s[n_cand + s])
        block = block.astype(jnp.bfloat16)
        for j in range(count):
            outs[j][:, s * width : (s + 1) * width] = block[j * share : (j + 1) * share, :]


def feed_forward(rows_in, gates, ups, downs):
    count, n_w = len(rows_in), len(gates)
    n_cand = n_w // 2
    share, model = rows_in[0].shape
    return pl.pallas_call(
        functools.partial(ffn_kernel, n_cand, count),
        out_shape=[jax.ShapeDtypeStruct((share, model), jnp.bfloat16)] * count,
        in_specs=[any_spec()] * (count + 3 * n_w),
        out_specs=[vmem_spec()] * count,
        scratch_shapes=[
            VMEM((share * count, model), jnp.bfloat16),
            VMEM((n_w,) + gates[0].shape, jnp.bfloat16),
            VMEM((n_w,) + ups[0].shape, jnp.bfloat16),
            VMEM((n_w,) + downs[0].shape, jnp.bfloat16),
            pltpu.SemaphoreType.DMA((count + 3 * n_w,)),
        ],
        name="feed_forward",
    )(*rows_in, *gates, *ups, *downs)


def vocab_kernel(n_cand, count, n_src, first, end, start_ref, gold_ref, *refs):
    n_w = 2 * n_cand
    rows_in = refs[:count]
    weights = refs[count : count + n_w]
    carried = refs[count + n_w : count + n_w + n_src]
    out_ref, acts = refs[count + n_w + n_src :]
    step = pl.program_id(0)
    share = rows_in[0].shape[0]
    rows = share * count

    @pl.when(step == 0)
    def _():
        for j in range(count):
            acts[j * share : (j + 1) * share, :] = rows_in[j][...]
        if n_src:
            out_ref[...] = carried[0][...]
        else:
            out_ref[0] = jnp.full((8, rows), NEG, jnp.float32)
            out_ref[1] = jnp.zeros((8, rows), jnp.float32)
            out_ref[2] = jnp.zeros((8, rows), jnp.float32)

    width, depth = weights[0].shape
    column = (first + step) * width + lax.broadcasted_iota(jnp.int32, (width, 1), 0)
    inside = column < end
    for side in range(2):
        logits = None
        for s in range(n_cand):
            term = dot32_t(weights[side * n_cand + s][...], acts[:, s * depth : (s + 1) * depth])
            logits = term if logits is None else logits + term
        hit = (column == gold_ref[...] - start_ref[side]) & inside
        picked = jnp.where(hit, logits, 0.0).reshape(width // 8, 8, rows)
        out_ref[2] += jnp.sum(picked, axis=0)
        logits = jnp.where(inside, logits, NEG).reshape(width // 8, 8, rows)
        old = out_ref[0]
        new = jnp.maximum(old, jnp.max(logits, axis=0))
        terms = jnp.sum(jnp.exp(logits - new[None]), axis=0)
        out_ref[1] = out_ref[1] * jnp.exp(old - new) + terms
        out_ref[0] = new


def vocab_scores(starts, gold, rows_in, weights, whole, begin, end, carried):
    count, n_w = len(rows_in), len(weights)
    n_cand = n_w // 2
    share, model = rows_in[0].shape
    depth = weights[0].shape[1]
    rows = share * count
    width = VOCAB_STEP
    first = begin // width
    constant = pl.BlockSpec((share, model), lambda i: (0, 0))
    stats = pl.BlockSpec((3, 8, rows), lambda i: (0, 0, 0))
    columns = [
        pl.BlockSpec((width, depth), lambda i: (first + i, 0))
        if is_whole
        else pl.BlockSpec((width, depth), lambda i: (i, 0))
        for is_whole in whole
    ]
    return pl.pallas_call(
        functools.partial(vocab_kernel, n_cand, count, len(carried), first, end),
        grid=(pl.cdiv(end - begin, width),),
        out_shape=jax.ShapeDtypeStruct((3, 8, rows), jnp.float32),
        in_specs=[smem_spec(), pl.BlockSpec((1, rows), lambda i: (0, 0))]
        + [constant] * count
        + columns
        + [stats] * len(carried),
        out_specs=stats,
        scratch_shapes=[VMEM((rows, model), jnp.bfloat16)],
        name="vocab_scores",
    )(starts, gold, *rows_in, *weights, *carried)


def body(
    dec_hidden,
    enc_keys,
    enc_values,
    enc_lengths,
    cand_counts,
    gold_ids,
    gain_cross,
    w_query,
    w_out,
    gain_ffn,
    w_in_gate,
    w_in_up,
    w_ffn_out,
    gain_final,
    w_vocab,
):
    queries, cand_dev, length, model = dec_hidden.shape
    n_tok, n_cand = lax.axis_size("tok"), lax.axis_size("cand")
    tok, cand = lax.axis_index("tok"), lax.axis_index("cand")
    core, chip = tok % 2, tok // 2
    chips = n_tok // 2
    rows = cand_dev * length
    share = rows // chips
    block = model // n_cand
    head_cols = w_query.shape[1]
    half = n_cand // 2
    assert queries == 2 and n_cand % 2 == 0 and n_tok % 4 == 0 and n_tok & (n_tok - 1) == 0

    def swap(a, k):
        return lax.ppermute(a, "tok", [(i, i ^ k) for i in range(n_tok)])

    def across(a, shift):
        return lax.ppermute(a, "cand", [(i, (i - shift) % n_cand) for i in range(n_cand)])

    def from_cands(a):
        return [a] + [across(a, s) for s in range(1, n_cand)]

    def with_partner(parts):
        own = swap(parts[0], 1)
        return parts + [own] + [swap(a, 1) for a in parts[1:]]

    def rolled(a):
        return jnp.concatenate(
            [
                lax.dynamic_slice_in_dim(a, ((cand + s) % n_cand) * block, block, a.ndim - 1)
                for s in range(n_cand)
            ],
            axis=-1,
        )

    def gather_rows(a):
        out = [None] * chips
        out[0] = a
        for j in range(2, chips, 2):
            out[j] = swap(a, 2 * j)
        for j in range(0, chips, 2):
            out[j + 1] = swap(out[j], 2)
        return out

    def scatter_rows(parts):
        order = [j for j in range(2, chips, 2)]
        order = order[1:] + order[:1] + [0]
        near = {j: swap(parts[j + 1], 2) for j in order}
        back = [parts[0], near[0]]
        for j in order[:-1]:
            pair = parts[j].astype(jnp.float32) + near[j].astype(jnp.float32)
            back.append(swap(pair.astype(jnp.bfloat16), 2 * j))
        return back

    query_at = cand // half

    pair = jnp.stack(
        [
            lax.dynamic_index_in_dim(enc_keys, query_at, 0, keepdims=False),
            lax.dynamic_index_in_dim(enc_values, query_at, 0, keepdims=False),
        ]
    )
    pair = pair.reshape(2, pair.shape[1], n_tok, head_cols).transpose(2, 0, 1, 3)
    key_values = lax.all_to_all(pair, "tok", 0, 0, tiled=True)

    query_parts = from_cands(w_query)
    out_parts = with_partner(from_cands(w_out))
    gate_parts = with_partner(from_cands(w_in_gate.T))
    up_parts = with_partner(from_cands(w_in_up.T))
    down_parts = with_partner(from_cands(w_ffn_out))
    vocab_all = w_vocab.T
    vocab_dev = vocab_all.shape[0]
    cut = pl.cdiv(vocab_dev, VOCAB_STEP) // 2 * VOCAB_STEP
    vocab_low, vocab_high = vocab_all[:cut], vocab_all[cut:]
    vocab_other = swap(vocab_all, 1)

    flat = rolled(dec_hidden.reshape(queries * rows, model))
    wide = flat.astype(jnp.float32)
    gain_first, gain_mid, gain_last = (
        rolled(g.reshape(1, model)) for g in (gain_cross, gain_ffn, gain_final)
    )
    squares = jnp.mean(wide * wide, axis=-1, keepdims=True)
    normed = (wide * lax.rsqrt(squares + NORM_EPS) * gain_first).astype(jnp.bfloat16)
    query = sum(
        dot32(normed[:, s * block : (s + 1) * block], query_parts[s]) for s in range(n_cand)
    ).astype(jnp.bfloat16)
    query = query.reshape(queries, rows, head_cols)
    mine = lax.dynamic_index_in_dim(query, query_at, 0, keepdims=False)
    other = lax.dynamic_index_in_dim(query, 1 - query_at, 0, keepdims=False)
    peer = across(other, half)
    straight = (core == query_at).astype(jnp.int32)
    live = jnp.stack([lax.dynamic_index_in_dim(enc_lengths, query_at, 0, keepdims=False), straight])
    live, vocab_low, vocab_high = lax.optimization_barrier((live, vocab_low, vocab_high))
    first, second = attention(live, mine, peer, key_values)

    def route(a, flip):
        perm = []
        for t in range(n_tok):
            for c in range(n_cand):
                to_half = (t % 2) ^ flip
                to = (t - t % 2 + c // half) * n_cand + c % half + to_half * half
                perm.append((t * n_cand + c, to))
        return lax.ppermute(a, ("tok", "cand"), perm)

    first, second = route(first, 0), route(second, 1)
    chip_at = jnp.stack([chip, straight])
    vocab_low = from_cands(vocab_low)[1:]
    vocab_high = from_cands(vocab_high)[1:]
    low = [vocab_all] + vocab_low + [vocab_other] + [swap(w, 1) for w in vocab_low]
    high = [vocab_all] + vocab_high + [vocab_other] + [swap(w, 1) for w in vocab_high]
    cross_terms = project(chip_at, first, second, out_parts, chips)
    cross_terms = scatter_rows(cross_terms)
    base = lax.dynamic_slice_in_dim(flat, core * rows + chip * share, share, 0)
    normed_ffn, after_cross = residual_norm(base, gain_mid, cross_terms, True)
    ffn_rows = gather_rows(normed_ffn)
    ffn_terms = feed_forward(ffn_rows, gate_parts, up_parts, down_parts)
    ffn_terms = scatter_rows(ffn_terms)
    (normed_final,) = residual_norm(after_cross, gain_last, ffn_terms, False)
    final_rows = gather_rows(normed_final)

    order = chip ^ jnp.arange(chips)
    gold = lax.dynamic_index_in_dim(gold_ids, core, 0, keepdims=False).reshape(chips, share)
    gold = gold[order].reshape(1, rows)
    starts = jnp.stack([tok * vocab_dev, (tok ^ 1) * vocab_dev])
    whole = ([True] + [False] * (n_cand - 1)) * 2
    stats = vocab_scores(starts, gold, final_rows, low, whole, 0, cut, [])
    stats = vocab_scores(starts, gold, final_rows, high, whole, cut, vocab_dev, [stats])
    top = jnp.max(stats[0], axis=0)
    stats = jnp.stack(
        [top, jnp.sum(stats[1] * jnp.exp(stats[0] - top), axis=0), jnp.sum(stats[2], axis=0)]
    )
    stats = stats.reshape(3, chips, share)[:, order].reshape(3, rows)
    k = 2
    while k < n_tok:
        theirs = swap(stats, k)
        top = jnp.maximum(stats[0], theirs[0])
        total = stats[1] * jnp.exp(stats[0] - top) + theirs[1] * jnp.exp(theirs[0] - top)
        stats = jnp.stack([top, total, stats[2] + theirs[2]])
        k *= 2
    logprob = stats[2] - stats[0] - jnp.log(stats[1])
    per_cand = jnp.mean(logprob.reshape(cand_dev, length), axis=1)
    both = jnp.stack([per_cand, swap(per_cand, 1)])
    both = jnp.where(core == 0, both, both[::-1])
    cand_index = cand * cand_dev + lax.iota(jnp.int32, cand_dev)
    valid = cand_index[None, :] < cand_counts[:, None]
    cand_scores = jnp.where(valid, both, 0.0)
    best = jnp.max(jnp.where(valid, both, NEG), axis=1)
    k = 1
    while k < n_cand:
        best = jnp.maximum(
            best, lax.ppermute(best, "cand", [(i, i ^ k) for i in range(n_cand)])
        )
        k *= 2
    return (cand_scores, best)


def solution(mesh):
    in_specs = (
        P(None, "cand", None, None),
        P(None, "tok", None),
        P(None, "tok", None),
        P(),
        P(),
        P(None, "cand", None),
        P(),
        P("cand", "tok"),
        P("tok", "cand"),
        P(),
        P("cand", "tok"),
        P("cand", "tok"),
        P("tok", "cand"),
        P(),
        P("cand", "tok"),
    )
    out_specs = (P(None, "cand"), P())
    return jax.shard_map(body, mesh=mesh, in_specs=in_specs, out_specs=out_specs, check_vma=False)
```

```python
import functools

import jax
import jax.numpy as jnp
from jax import lax
from jax.experimental import pallas as pl
from jax.experimental.pallas import tpu as pltpu
from jax.sharding import PartitionSpec as P


HEAD_DIM = 64
NORM_EPS = 0.25
NEG = -1e30


VMEM = pltpu.VMEM
SMEM = pltpu.SMEM


def vmem_spec():
    return pl.BlockSpec(memory_space=VMEM)


def smem_spec():
    return pl.BlockSpec(memory_space=SMEM)


def hbm_spec():
    return pl.BlockSpec(memory_space=pltpu.MemorySpace.HBM)


def dot32(a, b):
    return jnp.dot(a, b, preferred_element_type=jnp.float32)


def dot32_t(a, b):
    return lax.dot_general(a, b, (((1,), (1,)), ((), ())), preferred_element_type=jnp.float32)


def gelu_tanh(v):
    inner = 0.7978845608028654 * (v + 0.044715 * (v * v * v))
    return 0.5 * v * (1.0 + jnp.tanh(inner))


def by_heads_kernel(count, query_ref, keys_ref, values_ref, out_ref, sems):
    cols = out_ref.shape[3]
    copies = []
    for d in range(count):
        for k, ref in enumerate((keys_ref, values_ref)):
            copies.append(
                pltpu.make_async_copy(
                    ref.at[query_ref[0], :, pl.ds(d * cols, cols)], out_ref.at[d, k], sems.at[d, k]
                )
            )
            copies[-1].start()
    for copy in copies:
        copy.wait()


def by_heads(query, keys, values, count):
    src, model = keys.shape[1:]
    cols = model // count
    if cols % 128:
        pair = jnp.stack([lax.dynamic_index_in_dim(a, query[0], 0, False) for a in (keys, values)])
        return pair.reshape(2, src, count, cols).transpose(2, 0, 1, 3)
    return pl.pallas_call(
        functools.partial(by_heads_kernel, count),
        out_shape=jax.ShapeDtypeStruct((count, 2, src, cols), keys.dtype),
        in_specs=[smem_spec(), hbm_spec(), hbm_spec()],
        out_specs=vmem_spec(),
        scratch_shapes=[pltpu.SemaphoreType.DMA((count, 2))],
        compiler_params=pltpu.CompilerParams(vmem_limit_bytes=63 << 20),
        name="by_heads",
    )(query, keys, values)


def attention_kernel(live_ref, mine_ref, peer_ref, kv_ref, first_ref, second_ref):
    src = kv_ref.shape[0] * kv_ref.shape[2]
    cols = kv_ref.shape[3]
    keys = kv_ref[:, 0].reshape(src, cols)
    values = kv_ref[:, 1].reshape(src, cols)
    token = lax.broadcasted_iota(jnp.int32, (1, src), 1)
    bias = jnp.where(token < live_ref[0], 0.0, NEG).astype(jnp.float32)
    lane_head = lax.broadcasted_iota(jnp.int32, (1, cols), 1) // HEAD_DIM
    rows = mine_ref.shape[0]
    step = min(rows, 128)
    straight = live_ref[1] == 1
    for out_ref, one_ref, two_ref in (
        (first_ref, mine_ref, peer_ref),
        (second_ref, peer_ref, mine_ref),
    ):
        for start in range(0, rows, step):
            at = slice(start, start + step)
            q = jnp.where(straight, one_ref[at, :], two_ref[at, :])
            mixed = jnp.zeros((step, cols), jnp.float32)
            for head in range(cols // HEAD_DIM):
                q_head = jnp.where(lane_head == head, q, jnp.zeros_like(q))
                scores = dot32_t(q_head, keys) + bias
                row_max = jnp.max(scores, axis=-1, keepdims=True)
                weights = jnp.exp(scores - row_max)
                denominator = jnp.sum(weights, axis=-1, keepdims=True)
                head_out = dot32(weights.astype(jnp.bfloat16), values) / denominator
                mixed = jnp.where(lane_head == head, head_out, mixed)
            out_ref[at, :] = mixed.astype(jnp.bfloat16)


def attention(live, mine, peer, kv):
    rows, cols = mine.shape
    return pl.pallas_call(
        attention_kernel,
        out_shape=[jax.ShapeDtypeStruct((rows, cols), jnp.bfloat16)] * 2,
        in_specs=[smem_spec(), vmem_spec(), vmem_spec(), vmem_spec()],
        out_specs=[vmem_spec()] * 2,
        compiler_params=pltpu.CompilerParams(vmem_limit_bytes=24 << 20),
        name="attention",
    )(live, mine, peer, kv)


def project_kernel(n_cand, count, chip_ref, first_ref, second_ref, *refs):
    weights = refs[: 2 * n_cand]
    outs = refs[2 * n_cand : 2 * n_cand + count]
    own_s, par_s = refs[2 * n_cand + count :]
    share = first_ref.shape[0] // count
    straight = chip_ref[1] == 1
    for j in range(count):
        at = pl.multiple_of((chip_ref[0] ^ j) * share, share)
        to = slice(j * share, (j + 1) * share)
        first, second = first_ref[pl.ds(at, share), :], second_ref[pl.ds(at, share), :]
        own_s[to, :] = jnp.where(straight, first, second)
        par_s[to, :] = jnp.where(straight, second, first)
    own, par = own_s[...], par_s[...]
    width = weights[0].shape[1]
    for s in range(n_cand):
        block = dot32(own, weights[s][...]) + dot32(par, weights[n_cand + s][...])
        block = block.astype(jnp.bfloat16)
        for j in range(count):
            outs[j][:, s * width : (s + 1) * width] = block[j * share : (j + 1) * share, :]


def project(chip, first, second, weights, count):
    rows, cols = first.shape
    n_cand = len(weights) // 2
    model = weights[0].shape[1] * n_cand
    return pl.pallas_call(
        functools.partial(project_kernel, n_cand, count),
        out_shape=[jax.ShapeDtypeStruct((rows // count, model), jnp.bfloat16)] * count,
        in_specs=[smem_spec()] + [vmem_spec()] * (2 + len(weights)),
        out_specs=[vmem_spec()] * count,
        scratch_shapes=[VMEM((rows, cols), jnp.bfloat16)] * 2,
        compiler_params=pltpu.CompilerParams(vmem_limit_bytes=8 << 20),
        name="project",
    )(chip, first, second, *weights)


def residual_kernel(count, base_ref, gain_ref, *refs):
    total = base_ref[...].astype(jnp.float32)
    for part in refs[:count]:
        total = total + part[...].astype(jnp.float32)
    squares = jnp.mean(total * total, axis=-1, keepdims=True)
    refs[count][...] = (total * lax.rsqrt(squares + NORM_EPS) * gain_ref[...]).astype(jnp.bfloat16)
    if len(refs) > count + 1:
        refs[count + 1][...] = total


def residual_norm(base, gain, parts, keep):
    shapes = [jax.ShapeDtypeStruct(base.shape, jnp.bfloat16)]
    if keep:
        shapes.append(jax.ShapeDtypeStruct(base.shape, jnp.float32))
    return pl.pallas_call(
        functools.partial(residual_kernel, len(parts)),
        out_shape=shapes,
        in_specs=[vmem_spec()] * (2 + len(parts)),
        out_specs=[vmem_spec()] * len(shapes),
        compiler_params=pltpu.CompilerParams(vmem_limit_bytes=4 << 20),
        name="residual_norm",
    )(base, gain, *parts)


def ffn_kernel(n_cand, count, *refs):
    n_w = 2 * n_cand
    rows_in = refs[:count]
    gates = refs[count : count + n_w]
    ups = refs[count + n_w : count + 2 * n_w]
    downs = refs[count + 2 * n_w : count + 3 * n_w]
    outs = refs[count + 3 * n_w : 2 * count + 3 * n_w]
    acts = refs[2 * count + 3 * n_w]
    share = rows_in[0].shape[0]
    for j in range(count):
        acts[j * share : (j + 1) * share, :] = rows_in[j][...]
    depth = gates[0].shape[1]
    hidden = []
    for side in range(2):
        gate_part, up_part = None, None
        for s in range(n_cand):
            i = side * n_cand + s
            block = acts[:, s * depth : (s + 1) * depth]
            term = dot32_t(block, gates[i][...])
            gate_part = term if gate_part is None else gate_part + term
            term = dot32_t(block, ups[i][...])
            up_part = term if up_part is None else up_part + term
        hidden.append((gelu_tanh(gate_part) * up_part).astype(jnp.bfloat16))
    width = downs[0].shape[1]
    for s in range(n_cand):
        block = dot32(hidden[0], downs[s][...]) + dot32(hidden[1], downs[n_cand + s][...])
        block = block.astype(jnp.bfloat16)
        for j in range(count):
            outs[j][:, s * width : (s + 1) * width] = block[j * share : (j + 1) * share, :]


def feed_forward(rows_in, gates, ups, downs):
    count, n_w = len(rows_in), len(gates)
    n_cand = n_w // 2
    share, model = rows_in[0].shape
    return pl.pallas_call(
        functools.partial(ffn_kernel, n_cand, count),
        out_shape=[jax.ShapeDtypeStruct((share, model), jnp.bfloat16)] * count,
        in_specs=[vmem_spec()] * (count + 3 * n_w),
        out_specs=[vmem_spec()] * count,
        scratch_shapes=[VMEM((share * count, model), jnp.bfloat16)],
        compiler_params=pltpu.CompilerParams(vmem_limit_bytes=24 << 20),
        name="feed_forward",
    )(*rows_in, *gates, *ups, *downs)


def vocab_kernel(n_cand, count, width, live, flag_ref, gold_ref, *refs):
    rows_in = refs[: 2 * count]
    n_w = 2 * n_cand
    own = refs[2 * count : 2 * count + n_cand]
    swapped = refs[2 * count + n_cand : 2 * count + n_w]
    out_ref, acts, held, max_s, sum_s, gold_s, sems = refs[2 * count + n_w :]
    share = rows_in[0].shape[0]
    rows = 2 * count * share
    vocab, depth = own[0].shape
    slots = held.shape[0]
    chunks = [(at, min(width, vocab - at)) for at in range(0, vocab, width)]
    mine = flag_ref[0] == 1

    def copy(i, s, source):
        at, size = chunks[i]
        return pltpu.make_async_copy(
            source.at[pl.ds(at, size)], held.at[i % slots, s, pl.ds(0, size)], sems.at[i % slots, s]
        )

    def start(i):
        for s in range(n_cand):
            here, there = (own, swapped) if s == 0 else (swapped, own)

            @pl.when(mine)
            def _():
                copy(i, s, here[s]).start()

            @pl.when(jnp.logical_not(mine))
            def _():
                copy(i, s, there[s]).start()

    for i in range(min(slots, len(chunks))):
        start(i)
    for j in range(count):
        at = pl.multiple_of((flag_ref[2] ^ j) * share, share)
        acts[pl.ds(at, share), :] = rows_in[j][...]
        for s in range(n_cand):
            p = (s - n_cand // 2) % n_cand
            acts[pl.ds(at + rows // 2, share), s * depth : (s + 1) * depth] = rows_in[count + j][
                :, p * depth : (p + 1) * depth
            ]
    max_s[...] = jnp.full_like(max_s, NEG)
    sum_s[...] = jnp.zeros_like(sum_s)
    gold_s[...] = jnp.zeros_like(gold_s)
    for i, (first, size) in enumerate(chunks):
        logits = None
        for s in range(n_cand):
            copy(i, s, own[s]).wait()
            term = dot32_t(held[i % slots, s, :size], acts[:, s * depth : (s + 1) * depth])
            logits = term if logits is None else logits + term
        if i + slots < len(chunks):
            start(i + slots)
        column = first + lax.broadcasted_iota(jnp.int32, (size, 1), 0)
        hit = column == gold_ref[...] - flag_ref[1]
        if first + size > live:
            hit = hit & (column < live)
            logits = jnp.where(column < live, logits, NEG)
        picked = jnp.where(hit, logits, 0.0)
        gold_s[...] += jnp.sum(picked.reshape(size // 8, 8, rows), axis=0)
        logits = logits.reshape(size // 8, 8, rows)
        old = max_s[...]
        new = jnp.maximum(old, jnp.max(logits, axis=0))
        terms = jnp.sum(jnp.exp(logits - new[None]), axis=0)
        sum_s[...] = sum_s[...] * jnp.exp(old - new) + terms
        max_s[...] = new
    top = jnp.max(max_s[...], axis=0, keepdims=True)
    total = jnp.sum(sum_s[...] * jnp.exp(max_s[...] - top), axis=0, keepdims=True)
    gold = jnp.sum(gold_s[...], axis=0, keepdims=True)
    for k, value in enumerate((top, total, gold)):
        for i in range(rows // 128):
            out_ref[k, i : i + 1, :] = value[:, i * 128 : (i + 1) * 128]


def vocab_scores(flags, gold, rows_in, own, swapped, live):
    count, n_cand = len(rows_in) // 2, len(own)
    share, model = rows_in[0].shape
    vocab, depth = own[0].shape
    rows = share * count * 2
    slots = 3
    width = pl.cdiv(pl.cdiv(vocab, 3), 16) * 16
    assert rows % 256 == 0
    return pl.pallas_call(
        functools.partial(vocab_kernel, n_cand, count, width, live),
        out_shape=jax.ShapeDtypeStruct((3, rows // 128, 128), jnp.float32),
        in_specs=[smem_spec()] + [vmem_spec()] * (1 + len(rows_in)) + [hbm_spec()] * (2 * n_cand),
        out_specs=vmem_spec(),
        scratch_shapes=[
            VMEM((rows, model), jnp.bfloat16),
            VMEM((slots, n_cand, width, depth), jnp.bfloat16),
        ]
        + [VMEM((8, rows), jnp.float32)] * 3
        + [pltpu.SemaphoreType.DMA((slots, n_cand))],
        compiler_params=pltpu.CompilerParams(vmem_limit_bytes=60 << 20),
        name="vocab_scores",
    )(flags, gold, *rows_in, *own, *swapped)


def mean_kernel(length, info_ref, here_ref, there_ref, out_ref):
    middle = here_ref.shape[1] // 2
    sub = lax.broadcasted_iota(jnp.int32, (middle, 128), 0)
    row = sub * 128 + lax.broadcasted_iota(jnp.int32, (middle, 128), 1)
    lane = lax.broadcasted_iota(jnp.int32, (1, 128), 1)
    cands = middle * 128 // length
    best = jnp.full((1, 1), NEG, jnp.float32)
    for part in range(2):
        one, two = slice(part * middle, (part + 1) * middle), slice((1 - part) * middle, (2 - part) * middle)
        top_here, top_there = here_ref[0, one, :], there_ref[0, two, :]
        top = jnp.maximum(top_here, top_there)
        total = here_ref[1, one, :] * jnp.exp(top_here - top)
        total = total + there_ref[1, two, :] * jnp.exp(top_there - top)
        logprob = here_ref[2, one, :] + there_ref[2, two, :] - top - jnp.log(total)
        first = info_ref[1 + part]
        means = jnp.zeros((1, 128), jnp.float32)
        for c in range(cands):
            picked = jnp.where((row >= c * length) & (row < (c + 1) * length), logprob, 0.0)
            mean = jnp.sum(jnp.sum(picked, axis=0, keepdims=True), axis=1, keepdims=True) / length
            means = jnp.where(lane == c, mean, means)
            best = jnp.maximum(best, jnp.where(first + c < info_ref[0], mean, NEG))
        if part == 0:
            own = means
    out_ref[...] = jnp.where(lane < cands, own, best)


def candidate_means(info, here, there, length):
    return pl.pallas_call(
        functools.partial(mean_kernel, length),
        out_shape=jax.ShapeDtypeStruct((1, 128), jnp.float32),
        in_specs=[smem_spec(), vmem_spec(), vmem_spec()],
        out_specs=vmem_spec(),
        compiler_params=pltpu.CompilerParams(vmem_limit_bytes=2 << 20),
        name="candidate_means",
    )(info, here, there)


def result_kernel(info_ref, here_ref, there_ref, scores_ref, best_ref):
    cands = scores_ref.shape[1]
    low = info_ref[0] == 0
    here, there = here_ref[...], there_ref[...]
    lane = lax.broadcasted_iota(jnp.int32, (1, cands), 1) + info_ref[1]
    for q in range(2):
        line = jnp.where(low, here, there) if q == 0 else jnp.where(low, there, here)
        scores_ref[q : q + 1, :] = jnp.where(lane < info_ref[2 + q], line[:, :cands], 0.0)
        best_ref[:, q : q + 1] = line[:, cands : cands + 1]


def results(info, here, there, cands):
    return pl.pallas_call(
        result_kernel,
        out_shape=[
            jax.ShapeDtypeStruct((2, cands), jnp.float32),
            jax.ShapeDtypeStruct((1, 2), jnp.float32),
        ],
        in_specs=[smem_spec(), vmem_spec(), vmem_spec()],
        out_specs=[vmem_spec(), vmem_spec()],
        compiler_params=pltpu.CompilerParams(vmem_limit_bytes=2 << 20),
        name="results",
    )(info, here, there)


def body(
    dec_hidden,
    enc_keys,
    enc_values,
    enc_lengths,
    cand_counts,
    gold_ids,
    gain_cross,
    w_query,
    w_out,
    gain_ffn,
    w_in_gate,
    w_in_up,
    w_ffn_out,
    gain_final,
    w_vocab,
):
    queries, cand_dev, length, model = dec_hidden.shape
    n_tok, n_cand = lax.axis_size("tok"), lax.axis_size("cand")
    tok, cand = lax.axis_index("tok"), lax.axis_index("cand")
    core, chip = tok % 2, tok // 2
    chips = n_tok // 2
    rows = cand_dev * length
    half = n_cand // 2
    share = rows // chips
    block = model // n_cand
    head_cols = w_query.shape[1]
    assert queries == 2 and n_cand % 2 == 0 and n_tok % 4 == 0 and n_tok & (n_tok - 1) == 0

    def swap(a, k):
        return lax.ppermute(a, "tok", [(i, i ^ k) for i in range(n_tok)])

    def across(a, shift):
        return lax.ppermute(a, "cand", [(i, (i - shift) % n_cand) for i in range(n_cand)])

    def from_cands(a):
        return [a] + [across(a, s) for s in range(1, n_cand)]

    def with_partner(parts):
        own = swap(parts[0], 1)
        return parts + [own] + [swap(a, 1) for a in parts[1:]]

    def rolled(a):
        return jnp.concatenate(
            [
                lax.dynamic_slice_in_dim(a, ((cand + s) % n_cand) * block, block, a.ndim - 1)
                for s in range(n_cand)
            ],
            axis=-1,
        )

    def gather_rows(a, both):
        out, peer = [None] * chips, [None] * chips
        out[0] = a
        for j in range(2, chips, 2):
            out[j] = swap(a, 2 * j)
        for j in range(0, chips, 2):
            out[j + 1] = swap(out[j], 2)
        if not both:
            return out
        for j in range(chips):
            if j % 2 == 0 or j < chips // 2:
                peer[j] = across(out[j], half)
            else:
                peer[j] = swap(peer[j - 1], 2)
        return out + peer

    def scatter_rows(parts):
        order = [j for j in range(2, chips, 2)]
        order = order[1:] + order[:1] + [0]
        near = {j: swap(parts[j + 1], 2) for j in order}
        back = [parts[0], near[0]]
        for j in order[:-1]:
            pair = parts[j].astype(jnp.float32) + near[j].astype(jnp.float32)
            back.append(swap(pair.astype(jnp.bfloat16), 2 * j))
        return back

    query_at = cand // half

    pair = by_heads(query_at.reshape(1), enc_keys, enc_values, n_tok)
    key_values = lax.all_to_all(pair, "tok", 0, 0, tiled=True)

    query_parts = from_cands(w_query)
    out_parts = with_partner(from_cands(w_out))
    gate_parts = with_partner(from_cands(w_in_gate.T))
    up_parts = with_partner(from_cands(w_in_up.T))
    down_parts = with_partner(from_cands(w_ffn_out))
    vocab_dev = w_vocab.shape[1]
    vocab_own = w_vocab.T
    if vocab_dev % 8:
        vocab_own = jnp.pad(vocab_own, ((0, -vocab_dev % 8), (0, 0)))
    vocab_swapped = swap(vocab_own, 1)
    gold = lax.dynamic_index_in_dim(gold_ids, core, 0, keepdims=False).reshape(1, rows)
    gold = jnp.concatenate([gold, across(gold, half)], axis=1)

    flat = dec_hidden.reshape(queries * rows, model)
    base = rolled(lax.dynamic_slice_in_dim(flat, core * rows + chip * share, share, 0))
    flat = rolled(flat)
    wide = flat.astype(jnp.float32)
    gain_first, gain_mid, gain_last = (
        rolled(g.reshape(1, model)) for g in (gain_cross, gain_ffn, gain_final)
    )
    squares = jnp.mean(wide * wide, axis=-1, keepdims=True)
    normed = (wide * lax.rsqrt(squares + NORM_EPS) * gain_first).astype(jnp.bfloat16)
    query = sum(
        dot32(normed[:, s * block : (s + 1) * block], query_parts[s]) for s in range(n_cand)
    ).astype(jnp.bfloat16)
    query = query.reshape(queries, rows, head_cols)
    mine = lax.dynamic_index_in_dim(query, query_at, 0, keepdims=False)
    other = lax.dynamic_index_in_dim(query, 1 - query_at, 0, keepdims=False)
    peer = across(other, half)
    straight = (core == query_at).astype(jnp.int32)
    live = jnp.stack([lax.dynamic_index_in_dim(enc_lengths, query_at, 0, keepdims=False), straight])
    count_here = lax.dynamic_index_in_dim(cand_counts, core, 0, keepdims=False)
    plane_first, plane_other = cand * cand_dev, ((cand + half) % n_cand) * cand_dev
    mean_info = jnp.stack([count_here, plane_first, plane_other])
    result_info = jnp.stack([core, plane_first, cand_counts[0], cand_counts[1]])
    chip_at = jnp.stack([chip, straight])
    flags = jnp.stack([straight, (chip * 2 + query_at) * vocab_dev, chip])
    live, base, gain_mid, gain_last, gold, mean_info, result_info, chip_at, flags = (
        lax.optimization_barrier(
            (live, base, gain_mid, gain_last, gold, mean_info, result_info, chip_at, flags)
        )
    )
    first, second = attention(live, mine, peer, key_values)

    def route(a, flip):
        perm = []
        for t in range(n_tok):
            for c in range(n_cand):
                to_half = (t % 2) ^ flip
                to = (t - t % 2 + c // half) * n_cand + c % half + to_half * half
                perm.append((t * n_cand + c, to))
        return lax.ppermute(a, ("tok", "cand"), perm)

    first, second = route(first, 0), route(second, 1)
    vocab_own = [vocab_own]
    for s in range(1, n_cand):
        perm = []
        for c in range(n_cand):
            side = c // half
            for t in range(0, n_tok, 2):
                perm.append(((t + side) * n_cand + (c + s) % n_cand, (t + 1 - side) * n_cand + c))
        vocab_own.append(lax.ppermute(vocab_own[0], ("tok", "cand"), perm))
    vocab_swapped = [vocab_swapped] + [swap(w, 1) for w in vocab_own[1:]]
    cross_terms = project(chip_at, first, second, out_parts, chips)
    cross_terms = scatter_rows(cross_terms)
    normed_ffn, after_cross = residual_norm(base, gain_mid, cross_terms, True)
    ffn_rows = gather_rows(normed_ffn, False)
    ffn_terms = feed_forward(ffn_rows, gate_parts, up_parts, down_parts)
    ffn_terms = scatter_rows(ffn_terms)
    (normed_final,) = residual_norm(after_cross, gain_last, ffn_terms, False)
    final_rows = gather_rows(normed_final, True)

    stats = vocab_scores(flags, gold, final_rows, vocab_own, vocab_swapped, vocab_dev)

    def combine(parts):
        top = functools.reduce(jnp.maximum, [p[0] for p in parts])
        total = sum(p[1] * jnp.exp(p[0] - top) for p in parts)
        return jnp.stack([top, total, sum(p[2] for p in parts)])

    stats = combine([stats, swap(stats, 2)])
    stats = combine([stats] + [swap(stats, 2 * j) for j in range(2, chips, 2)])
    theirs = across(stats, half)
    means = candidate_means(mean_info, stats, theirs, length)
    k = 1
    while k < half:
        other_best = lax.ppermute(means, "cand", [(i, i ^ k) for i in range(n_cand)])
        past = lax.iota(jnp.int32, 128)[None, :] >= cand_dev
        means = jnp.where(past, jnp.maximum(means, other_best), means)
        k *= 2
    cand_scores, best = results(result_info, means, swap(means, 1), cand_dev)
    return (cand_scores, best.reshape(2))


def solution(mesh):
    in_specs = (
        P(None, "cand", None, None),
        P(None, "tok", None),
        P(None, "tok", None),
        P(),
        P(),
        P(None, "cand", None),
        P(),
        P("cand", "tok"),
        P("tok", "cand"),
        P(),
        P("cand", "tok"),
        P("cand", "tok"),
        P("tok", "cand"),
        P(),
        P("cand", "tok"),
    )
    out_specs = (P(None, "cand"), P())
    return jax.shard_map(body, mesh=mesh, in_specs=in_specs, out_specs=out_specs, check_vma=False)
```

```python
import functools

import jax
import jax.numpy as jnp
from jax import lax
from jax.experimental import pallas as pl
from jax.experimental.pallas import tpu as pltpu
from jax.sharding import PartitionSpec as P


HEAD_DIM = 64
NORM_EPS = 0.25
NEG = -1e30


VMEM = pltpu.VMEM
SMEM = pltpu.SMEM


def vmem_spec():
    return pl.BlockSpec(memory_space=VMEM)


def smem_spec():
    return pl.BlockSpec(memory_space=SMEM)


def hbm_spec():
    return pl.BlockSpec(memory_space=pltpu.MemorySpace.HBM)


def place(n_cand):
    tok = lax.axis_index("tok")
    return tok % 2, tok // 2, lax.axis_index("cand") // (n_cand // 2)


def dot32(a, b):
    return jnp.dot(a, b, preferred_element_type=jnp.float32)


def dot32_t(a, b):
    return lax.dot_general(a, b, (((1,), (1,)), ((), ())), preferred_element_type=jnp.float32)


def gelu_tanh(v):
    inner = 0.7978845608028654 * (v + 0.044715 * (v * v * v))
    return 0.5 * v * (1.0 + jnp.tanh(inner))


def by_heads_kernel(count, n_cand, keys_ref, values_ref, out_ref, sems):
    query_at = place(n_cand)[2]
    cols = out_ref.shape[3]
    copies = []
    for d in range(count):
        for k, ref in enumerate((keys_ref, values_ref)):
            copies.append(
                pltpu.make_async_copy(
                    ref.at[query_at, :, pl.ds(d * cols, cols)], out_ref.at[d, k], sems.at[d, k]
                )
            )
            copies[-1].start()
    for copy in copies:
        copy.wait()


def by_heads(query, keys, values, count, n_cand):
    src, model = keys.shape[1:]
    cols = model // count
    if cols % 128:
        pair = jnp.stack([lax.dynamic_index_in_dim(a, query, 0, False) for a in (keys, values)])
        return pair.reshape(2, src, count, cols).transpose(2, 0, 1, 3)
    return pl.pallas_call(
        functools.partial(by_heads_kernel, count, n_cand),
        out_shape=jax.ShapeDtypeStruct((count, 2, src, cols), keys.dtype),
        in_specs=[hbm_spec(), hbm_spec()],
        out_specs=vmem_spec(),
        scratch_shapes=[pltpu.SemaphoreType.DMA((count, 2))],
        compiler_params=pltpu.CompilerParams(vmem_limit_bytes=63 << 20),
        name="by_heads",
    )(keys, values)


def attention_kernel(n_cand, lengths_ref, mine_ref, peer_ref, kv_ref, first_ref, second_ref):
    core, _, query_at = place(n_cand)
    straight = core == query_at
    src = kv_ref.shape[0] * kv_ref.shape[2]
    cols = kv_ref.shape[3]
    keys = kv_ref[:, 0].reshape(src, cols)
    values = kv_ref[:, 1].reshape(src, cols)
    token = lax.broadcasted_iota(jnp.int32, (1, src), 1)
    bias = jnp.where(token < lengths_ref[query_at], 0.0, NEG).astype(jnp.float32)
    lane_head = lax.broadcasted_iota(jnp.int32, (1, cols), 1) // HEAD_DIM
    rows = mine_ref.shape[0]
    step = min(rows, 256)
    for out_ref, one_ref, two_ref in (
        (first_ref, mine_ref, peer_ref),
        (second_ref, peer_ref, mine_ref),
    ):
        for start in range(0, rows, step):
            at = slice(start, start + step)
            q = jnp.where(straight, one_ref[at, :], two_ref[at, :])
            mixed = jnp.zeros((step, cols), jnp.float32)
            for head in range(cols // HEAD_DIM):
                q_head = jnp.where(lane_head == head, q, jnp.zeros_like(q))
                scores = dot32_t(q_head, keys) + bias
                row_max = jnp.max(scores, axis=-1, keepdims=True)
                weights = jnp.exp(scores - row_max)
                denominator = jnp.sum(weights, axis=-1, keepdims=True)
                head_out = dot32(weights.astype(jnp.bfloat16), values) / denominator
                mixed = jnp.where(lane_head == head, head_out, mixed)
            out_ref[at, :] = mixed.astype(jnp.bfloat16)


def attention(lengths, mine, peer, kv, n_cand):
    rows, cols = mine.shape
    return pl.pallas_call(
        functools.partial(attention_kernel, n_cand),
        out_shape=[jax.ShapeDtypeStruct((rows, cols), jnp.bfloat16)] * 2,
        in_specs=[smem_spec(), vmem_spec(), vmem_spec(), vmem_spec()],
        out_specs=[vmem_spec()] * 2,
        compiler_params=pltpu.CompilerParams(vmem_limit_bytes=24 << 20),
        name="attention",
    )(lengths, mine, peer, kv)


def project_kernel(n_cand, count, first_ref, second_ref, *refs):
    weights = refs[: 2 * n_cand]
    outs = refs[2 * n_cand : 2 * n_cand + count]
    own_s, par_s = refs[2 * n_cand + count :]
    share = first_ref.shape[0] // count
    core, chip, query_at = place(n_cand)
    straight = core == query_at
    for j in range(count):
        at = pl.multiple_of((chip ^ j) * share, share)
        to = slice(j * share, (j + 1) * share)
        first, second = first_ref[pl.ds(at, share), :], second_ref[pl.ds(at, share), :]
        own_s[to, :] = jnp.where(straight, first, second)
        par_s[to, :] = jnp.where(straight, second, first)
    own, par = own_s[...], par_s[...]
    width = weights[0].shape[1]
    for s in range(n_cand):
        block = dot32(own, weights[s][...]) + dot32(par, weights[n_cand + s][...])
        block = block.astype(jnp.bfloat16)
        for j in range(count):
            outs[j][:, s * width : (s + 1) * width] = block[j * share : (j + 1) * share, :]


def project(first, second, weights, count):
    rows, cols = first.shape
    n_cand = len(weights) // 2
    model = weights[0].shape[1] * n_cand
    return pl.pallas_call(
        functools.partial(project_kernel, n_cand, count),
        out_shape=[jax.ShapeDtypeStruct((rows // count, model), jnp.bfloat16)] * count,
        in_specs=[vmem_spec()] * (2 + len(weights)),
        out_specs=[vmem_spec()] * count,
        scratch_shapes=[VMEM((rows, cols), jnp.bfloat16)] * 2,
        compiler_params=pltpu.CompilerParams(vmem_limit_bytes=8 << 20),
        name="project",
    )(first, second, *weights)


def residual_kernel(count, n_cand, base_ref, gain_ref, *refs):
    total = base_ref[...].astype(jnp.float32)
    for part in refs[:count]:
        total = total + part[...].astype(jnp.float32)
    squares = jnp.mean(total * total, axis=-1, keepdims=True)
    scaled = total * lax.rsqrt(squares + NORM_EPS)
    block = base_ref.shape[1] // n_cand
    for s in range(n_cand):
        at = pl.multiple_of(lax.rem(lax.axis_index("cand") + s, n_cand) * block, block)
        to = slice(s * block, (s + 1) * block)
        refs[count][:, to] = (scaled[:, to] * gain_ref[:, pl.ds(at, block)]).astype(jnp.bfloat16)
    if len(refs) > count + 1:
        refs[count + 1][...] = total


def residual_norm(base, gain, parts, n_cand, keep):
    shapes = [jax.ShapeDtypeStruct(base.shape, jnp.bfloat16)]
    if keep:
        shapes.append(jax.ShapeDtypeStruct(base.shape, jnp.float32))
    return pl.pallas_call(
        functools.partial(residual_kernel, len(parts), n_cand),
        out_shape=shapes,
        in_specs=[vmem_spec()] * (2 + len(parts)),
        out_specs=[vmem_spec()] * len(shapes),
        compiler_params=pltpu.CompilerParams(vmem_limit_bytes=4 << 20),
        name="residual_norm",
    )(base, gain.reshape(1, -1), *parts)


def ffn_kernel(n_cand, count, *refs):
    n_w = 2 * n_cand
    rows_in = refs[:count]
    gates = refs[count : count + n_w]
    ups = refs[count + n_w : count + 2 * n_w]
    downs = refs[count + 2 * n_w : count + 3 * n_w]
    outs = refs[count + 3 * n_w : 2 * count + 3 * n_w]
    acts = refs[2 * count + 3 * n_w]
    share = rows_in[0].shape[0]
    for j in range(count):
        acts[j * share : (j + 1) * share, :] = rows_in[j][...]
    depth = gates[0].shape[1]
    hidden = []
    for side in range(2):
        gate_part, up_part = None, None
        for s in range(n_cand):
            i = side * n_cand + s
            block = acts[:, s * depth : (s + 1) * depth]
            term = dot32_t(gates[i][...], block)
            gate_part = term if gate_part is None else gate_part + term
            term = dot32_t(ups[i][...], block)
            up_part = term if up_part is None else up_part + term
        hidden.append((gelu_tanh(gate_part) * up_part).astype(jnp.bfloat16).T)
    width = downs[0].shape[1]
    for s in range(n_cand):
        block = dot32(hidden[0], downs[s][...]) + dot32(hidden[1], downs[n_cand + s][...])
        block = block.astype(jnp.bfloat16)
        for j in range(count):
            outs[j][:, s * width : (s + 1) * width] = block[j * share : (j + 1) * share, :]


def feed_forward(rows_in, gates, ups, downs):
    count, n_w = len(rows_in), len(gates)
    n_cand = n_w // 2
    share, model = rows_in[0].shape
    return pl.pallas_call(
        functools.partial(ffn_kernel, n_cand, count),
        out_shape=[jax.ShapeDtypeStruct((share, model), jnp.bfloat16)] * count,
        in_specs=[vmem_spec()] * (count + 3 * n_w),
        out_specs=[vmem_spec()] * count,
        scratch_shapes=[VMEM((share * count, model), jnp.bfloat16)],
        compiler_params=pltpu.CompilerParams(vmem_limit_bytes=24 << 20),
        name="feed_forward",
    )(*rows_in, *gates, *ups, *downs)


def vocab_kernel(n_cand, count, width, live, gold_ref, over_gold_ref, *refs):
    here, over = refs[:count], refs[count : 2 * count]
    own, swapped = refs[2 * count : 2 * count + n_cand], refs[2 * count + n_cand : -5]
    out_ref, acts, max_s, sum_s, gold_s = refs[-5:]
    share = here[0].shape[0]
    rows = 2 * count * share
    vocab, depth = own[0].shape
    core, chip, query_at = place(n_cand)
    mine = core == query_at
    start = (chip * 2 + query_at) * live
    gold_row = jnp.concatenate([gold_ref[...], over_gold_ref[...]], axis=1) - start
    for j in range(count):
        at = pl.multiple_of((chip ^ j) * share, share)
        acts[pl.ds(at, share), :] = here[j][...]
        for s in range(n_cand):
            p = (s - n_cand // 2) % n_cand
            acts[pl.ds(at + rows // 2, share), s * depth : (s + 1) * depth] = over[j][
                :, p * depth : (p + 1) * depth
            ]
    max_s[...] = jnp.full_like(max_s, NEG)
    sum_s[...] = jnp.zeros_like(sum_s)
    gold_s[...] = jnp.zeros_like(gold_s)
    for first in range(0, vocab, width):
        size = min(width, vocab - first)
        logits = None
        for s in range(n_cand):
            one, two = (own, swapped) if s == 0 else (swapped, own)
            at = slice(first, first + size)
            part = jnp.where(mine, one[s][at, :], two[s][at, :])
            term = dot32_t(part, acts[:, s * depth : (s + 1) * depth])
            logits = term if logits is None else logits + term
        column = first + lax.broadcasted_iota(jnp.int32, (size, 1), 0)
        hit = column == gold_row
        if first + size > live:
            hit = hit & (column < live)
            logits = jnp.where(column < live, logits, NEG)
        picked = jnp.where(hit, logits, 0.0)
        gold_s[...] += jnp.sum(picked.reshape(size // 8, 8, rows), axis=0)
        logits = logits.reshape(size // 8, 8, rows)
        old = max_s[...]
        new = jnp.maximum(old, jnp.max(logits, axis=0))
        terms = jnp.sum(jnp.exp(logits - new[None]), axis=0)
        sum_s[...] = sum_s[...] * jnp.exp(old - new) + terms
        max_s[...] = new
    top = jnp.max(max_s[...], axis=0, keepdims=True)
    total = jnp.sum(sum_s[...] * jnp.exp(max_s[...] - top), axis=0, keepdims=True)
    gold = jnp.sum(gold_s[...], axis=0, keepdims=True)
    for k, value in enumerate((top, total, gold)):
        for i in range(rows // 128):
            out_ref[k, i : i + 1, :] = value[:, i * 128 : (i + 1) * 128]


def vocab_scores(gold, over_gold, rows_in, own, swapped, live):
    count, n_cand = len(rows_in) // 2, len(own)
    share, model = rows_in[0].shape
    vocab = own[0].shape[0]
    rows = share * count * 2
    width = pl.cdiv(pl.cdiv(vocab, 3), 16) * 16
    assert rows % 256 == 0
    operands = (gold, over_gold, *rows_in, *own, *swapped)
    return pl.pallas_call(
        functools.partial(vocab_kernel, n_cand, count, width, live),
        out_shape=jax.ShapeDtypeStruct((3, rows // 128, 128), jnp.float32),
        in_specs=[vmem_spec()] * len(operands),
        out_specs=vmem_spec(),
        scratch_shapes=[VMEM((rows, model), jnp.bfloat16)] + [VMEM((8, rows), jnp.float32)] * 3,
        compiler_params=pltpu.CompilerParams(vmem_limit_bytes=20 << 20),
        name="vocab_scores",
    )(*operands)


def mean_kernel(length, n_cand, counts_ref, here_ref, there_ref, out_ref):
    core = place(n_cand)[0]
    cand = lax.axis_index("cand")
    middle = here_ref.shape[1] // 2
    sub = lax.broadcasted_iota(jnp.int32, (middle, 128), 0)
    row = sub * 128 + lax.broadcasted_iota(jnp.int32, (middle, 128), 1)
    lane = lax.broadcasted_iota(jnp.int32, (1, 128), 1)
    cands = middle * 128 // length
    best = jnp.full((1, 1), NEG, jnp.float32)
    for part in range(2):
        one, two = slice(part * middle, (part + 1) * middle), slice((1 - part) * middle, (2 - part) * middle)
        top_here, top_there = here_ref[0, one, :], there_ref[0, two, :]
        top = jnp.maximum(top_here, top_there)
        total = here_ref[1, one, :] * jnp.exp(top_here - top)
        total = total + there_ref[1, two, :] * jnp.exp(top_there - top)
        logprob = here_ref[2, one, :] + there_ref[2, two, :] - top - jnp.log(total)
        first = lax.rem(cand + part * (n_cand // 2), n_cand) * cands
        means = jnp.zeros((1, 128), jnp.float32)
        for c in range(cands):
            picked = jnp.where((row >= c * length) & (row < (c + 1) * length), logprob, 0.0)
            mean = jnp.sum(jnp.sum(picked, axis=0, keepdims=True), axis=1, keepdims=True) / length
            means = jnp.where(lane == c, mean, means)
            best = jnp.maximum(best, jnp.where(first + c < counts_ref[core], mean, NEG))
        if part == 0:
            own = means
    out_ref[...] = jnp.where(lane < cands, own, best)


def candidate_means(counts, here, there, length, n_cand):
    return pl.pallas_call(
        functools.partial(mean_kernel, length, n_cand),
        out_shape=jax.ShapeDtypeStruct((1, 128), jnp.float32),
        in_specs=[smem_spec(), vmem_spec(), vmem_spec()],
        out_specs=vmem_spec(),
        compiler_params=pltpu.CompilerParams(vmem_limit_bytes=2 << 20),
        name="candidate_means",
    )(counts, here, there)


def result_kernel(n_cand, counts_ref, here_ref, there_ref, scores_ref, best_ref):
    cands = scores_ref.shape[1]
    low = place(n_cand)[0] == 0
    here, there = here_ref[...], there_ref[...]
    lane = lax.broadcasted_iota(jnp.int32, (1, cands), 1) + lax.axis_index("cand") * cands
    for q in range(2):
        line = jnp.where(low, here, there) if q == 0 else jnp.where(low, there, here)
        scores_ref[q : q + 1, :] = jnp.where(lane < counts_ref[q], line[:, :cands], 0.0)
        best_ref[:, q : q + 1] = line[:, cands : cands + 1]


def results(counts, here, there, cands, n_cand):
    return pl.pallas_call(
        functools.partial(result_kernel, n_cand),
        out_shape=[
            jax.ShapeDtypeStruct((2, cands), jnp.float32),
            jax.ShapeDtypeStruct((1, 2), jnp.float32),
        ],
        in_specs=[smem_spec(), vmem_spec(), vmem_spec()],
        out_specs=[vmem_spec(), vmem_spec()],
        compiler_params=pltpu.CompilerParams(vmem_limit_bytes=2 << 20),
        name="results",
    )(counts, here, there)


def body(
    dec_hidden,
    enc_keys,
    enc_values,
    enc_lengths,
    cand_counts,
    gold_ids,
    gain_cross,
    w_query,
    w_out,
    gain_ffn,
    w_in_gate,
    w_in_up,
    w_ffn_out,
    gain_final,
    w_vocab,
):
    queries, cand_dev, length, model = dec_hidden.shape
    n_tok, n_cand = lax.axis_size("tok"), lax.axis_size("cand")
    tok, cand = lax.axis_index("tok"), lax.axis_index("cand")
    core, chip = tok % 2, tok // 2
    chips = n_tok // 2
    rows = cand_dev * length
    half = n_cand // 2
    share = rows // chips
    block = model // n_cand
    head_cols = w_query.shape[1]
    assert queries == 2 and n_cand % 2 == 0 and n_tok % 4 == 0 and n_tok & (n_tok - 1) == 0

    def swap(a, k):
        return lax.ppermute(a, "tok", [(i, i ^ k) for i in range(n_tok)])

    def across(a, shift):
        return lax.ppermute(a, "cand", [(i, (i - shift) % n_cand) for i in range(n_cand)])

    def from_cands(a):
        return [a] + [across(a, s) for s in range(1, n_cand)]

    def with_partner(parts):
        own = swap(parts[0], 1)
        return parts + [own] + [swap(a, 1) for a in parts[1:]]

    def rolled(a):
        return jnp.concatenate(
            [
                lax.dynamic_slice_in_dim(a, ((cand + s) % n_cand) * block, block, a.ndim - 1)
                for s in range(n_cand)
            ],
            axis=-1,
        )

    def gather_rows(a, both=False):
        out, over = [None] * chips, [None] * chips
        out[0] = a
        for j in range(2, chips, 2):
            out[j] = swap(a, 2 * j)
        for j in range(0, chips, 2):
            out[j + 1] = swap(out[j], 2)
        if not both:
            return out
        for j in range(chips):
            if j % 2 == 0:
                over[j] = across(out[j], half)
            else:
                over[j] = swap(over[j - 1], 2)
        return out + over

    def scatter_rows(parts):
        order = [j for j in range(4, chips, 2)] + [2, 0]
        near = {j: swap(parts[j + 1], 2) for j in order}
        back = [parts[0], near[0]]
        for j in order[:-1]:
            pair = parts[j].astype(jnp.float32) + near[j].astype(jnp.float32)
            back.append(swap(pair.astype(jnp.bfloat16), 2 * j))
        return back

    query_at = cand // half

    pair = by_heads(query_at, enc_keys, enc_values, n_tok, n_cand)
    key_values = lax.all_to_all(pair, "tok", 0, 0, tiled=True)

    query_parts = from_cands(w_query)
    out_parts = with_partner(from_cands(w_out))
    gate_parts = with_partner(from_cands(w_in_gate.T))
    up_parts = with_partner(from_cands(w_in_up.T))
    down_parts = with_partner(from_cands(w_ffn_out))
    vocab_dev = w_vocab.shape[1]
    vocab_own = w_vocab.T
    if vocab_dev % 8:
        vocab_own = jnp.pad(vocab_own, ((0, -vocab_dev % 8), (0, 0)))
    vocab_swapped = swap(vocab_own, 1)
    gold = lax.dynamic_index_in_dim(gold_ids, core, 0, keepdims=False).reshape(1, rows)
    over_gold = across(gold, half)

    flat = dec_hidden.reshape(queries * rows, model)
    base = rolled(lax.dynamic_slice_in_dim(flat, core * rows + chip * share, share, 0))
    flat = rolled(flat)
    wide = flat.astype(jnp.float32)
    gain_first = rolled(gain_cross.reshape(1, model))
    squares = jnp.mean(wide * wide, axis=-1, keepdims=True)
    normed = (wide * lax.rsqrt(squares + NORM_EPS) * gain_first).astype(jnp.bfloat16)
    query = sum(
        dot32(normed[:, s * block : (s + 1) * block], query_parts[s]) for s in range(n_cand)
    ).astype(jnp.bfloat16)
    query = query.reshape(queries, rows, head_cols)
    mine = lax.dynamic_index_in_dim(query, query_at, 0, keepdims=False)
    other = lax.dynamic_index_in_dim(query, 1 - query_at, 0, keepdims=False)
    peer = across(other, half)
    mine, base, gold, over_gold = lax.optimization_barrier((mine, base, gold, over_gold))
    first, second = attention(enc_lengths, mine, peer, key_values, n_cand)

    def route(a, flip):
        perm = []
        for t in range(n_tok):
            for c in range(n_cand):
                to_half = (t % 2) ^ flip
                to = (t - t % 2 + c // half) * n_cand + c % half + to_half * half
                perm.append((t * n_cand + c, to))
        return lax.ppermute(a, ("tok", "cand"), perm)

    first, second = route(first, 0), route(second, 1)
    vocab_own = [vocab_own]
    for s in range(1, n_cand):
        perm = []
        for c in range(n_cand):
            side = c // half
            for t in range(0, n_tok, 2):
                perm.append(((t + side) * n_cand + (c + s) % n_cand, (t + 1 - side) * n_cand + c))
        vocab_own.append(lax.ppermute(vocab_own[0], ("tok", "cand"), perm))
    vocab_swapped = [vocab_swapped] + [swap(w, 1) for w in vocab_own[1:]]
    cross_terms = project(first, second, out_parts, chips)
    cross_terms = scatter_rows(cross_terms)
    normed_ffn, after_cross = residual_norm(base, gain_ffn, cross_terms, n_cand, True)
    ffn_rows = gather_rows(normed_ffn)
    ffn_terms = feed_forward(ffn_rows, gate_parts, up_parts, down_parts)
    ffn_terms = scatter_rows(ffn_terms)
    (normed_final,) = residual_norm(after_cross, gain_final, ffn_terms, n_cand, False)
    final_rows = gather_rows(normed_final, True)

    stats = vocab_scores(
        gold, over_gold, final_rows, vocab_own, vocab_swapped, vocab_dev
    )

    def combine(parts):
        top = functools.reduce(jnp.maximum, [p[0] for p in parts])
        total = sum(p[1] * jnp.exp(p[0] - top) for p in parts)
        return jnp.stack([top, total, sum(p[2] for p in parts)])

    stats = combine([stats, swap(stats, 2)])
    stats = combine([stats] + [swap(stats, 2 * j) for j in range(2, chips, 2)])
    theirs = across(stats, half)
    means = candidate_means(cand_counts, stats, theirs, length, n_cand)
    k = 1
    while k < half:
        other_best = lax.ppermute(means, "cand", [(i, i ^ k) for i in range(n_cand)])
        past = lax.iota(jnp.int32, 128)[None, :] >= cand_dev
        means = jnp.where(past, jnp.maximum(means, other_best), means)
        k *= 2
    cand_scores, best = results(cand_counts, means, swap(means, 1), cand_dev, n_cand)
    return (cand_scores, best.reshape(2))


def solution(mesh):
    in_specs = (
        P(None, "cand", None, None),
        P(None, "tok", None),
        P(None, "tok", None),
        P(),
        P(),
        P(None, "cand", None),
        P(),
        P("cand", "tok"),
        P("tok", "cand"),
        P(),
        P("cand", "tok"),
        P("cand", "tok"),
        P("tok", "cand"),
        P(),
        P("cand", "tok"),
    )
    out_specs = (P(None, "cand"), P())
    return jax.shard_map(body, mesh=mesh, in_specs=in_specs, out_specs=out_specs, check_vma=False)
```

```python
import functools

import jax
import jax.numpy as jnp
from jax import lax
from jax.experimental import pallas as pl
from jax.experimental.pallas import tpu as pltpu
from jax.sharding import PartitionSpec as P


HEAD_DIM = 64
NORM_EPS = 0.25
NEG = -1e30


VMEM = pltpu.VMEM
SMEM = pltpu.SMEM


def vmem_spec():
    return pl.BlockSpec(memory_space=VMEM)


def smem_spec():
    return pl.BlockSpec(memory_space=SMEM)


def hbm_spec():
    return pl.BlockSpec(memory_space=pltpu.MemorySpace.HBM)


def place(n_cand):
    tok = lax.axis_index("tok")
    return tok % 2, tok // 2, lax.axis_index("cand") // (n_cand // 2)


def dot32(a, b):
    return jnp.dot(a, b, preferred_element_type=jnp.float32)


def dot32_t(a, b):
    return lax.dot_general(a, b, (((1,), (1,)), ((), ())), preferred_element_type=jnp.float32)


def gelu_tanh(v):
    inner = 0.7978845608028654 * (v + 0.044715 * (v * v * v))
    return 0.5 * v * (1.0 + jnp.tanh(inner))


def by_heads_kernel(count, n_cand, keys_ref, values_ref, out_ref, sems):
    query_at = place(n_cand)[2]
    cols = out_ref.shape[3]
    copies = []
    for d in range(count):
        for k, ref in enumerate((keys_ref, values_ref)):
            copies.append(
                pltpu.make_async_copy(
                    ref.at[query_at, :, pl.ds(d * cols, cols)], out_ref.at[d, k], sems.at[d, k]
                )
            )
            copies[-1].start()
    for copy in copies:
        copy.wait()


def by_heads(query, keys, values, count, n_cand):
    src, model = keys.shape[1:]
    cols = model // count
    if cols % 128:
        pair = jnp.stack([lax.dynamic_index_in_dim(a, query, 0, False) for a in (keys, values)])
        return pair.reshape(2, src, count, cols).transpose(2, 0, 1, 3)
    return pl.pallas_call(
        functools.partial(by_heads_kernel, count, n_cand),
        out_shape=jax.ShapeDtypeStruct((count, 2, src, cols), keys.dtype),
        in_specs=[hbm_spec(), hbm_spec()],
        out_specs=vmem_spec(),
        scratch_shapes=[pltpu.SemaphoreType.DMA((count, 2))],
        compiler_params=pltpu.CompilerParams(vmem_limit_bytes=63 << 20),
        name="by_heads",
    )(keys, values)


def attention_kernel(n_cand, lengths_ref, mine_ref, peer_ref, kv_ref, first_ref, second_ref):
    core, _, query_at = place(n_cand)
    straight = core == query_at
    src = kv_ref.shape[0] * kv_ref.shape[2]
    cols = kv_ref.shape[3]
    keys = kv_ref[:, 0].reshape(src, cols)
    values = kv_ref[:, 1].reshape(src, cols)
    token = lax.broadcasted_iota(jnp.int32, (1, src), 1)
    bias = jnp.where(token < lengths_ref[query_at], 0.0, NEG).astype(jnp.float32)
    lane_head = lax.broadcasted_iota(jnp.int32, (1, cols), 1) // HEAD_DIM
    rows = mine_ref.shape[0]
    step = min(rows, 256)
    for out_ref, one_ref, two_ref in (
        (first_ref, mine_ref, peer_ref),
        (second_ref, peer_ref, mine_ref),
    ):
        for start in range(0, rows, step):
            at = slice(start, start + step)
            q = jnp.where(straight, one_ref[at, :], two_ref[at, :])
            mixed = jnp.zeros((step, cols), jnp.float32)
            for head in range(cols // HEAD_DIM):
                q_head = jnp.where(lane_head == head, q, jnp.zeros_like(q))
                scores = dot32_t(q_head, keys) + bias
                row_max = jnp.max(scores, axis=-1, keepdims=True)
                weights = jnp.exp(scores - row_max)
                denominator = jnp.sum(weights, axis=-1, keepdims=True)
                head_out = dot32(weights.astype(jnp.bfloat16), values) / denominator
                mixed = jnp.where(lane_head == head, head_out, mixed)
            out_ref[at, :] = mixed.astype(jnp.bfloat16)


def attention(lengths, mine, peer, kv, n_cand):
    rows, cols = mine.shape
    return pl.pallas_call(
        functools.partial(attention_kernel, n_cand),
        out_shape=[jax.ShapeDtypeStruct((rows, cols), jnp.bfloat16)] * 2,
        in_specs=[smem_spec(), vmem_spec(), vmem_spec(), vmem_spec()],
        out_specs=[vmem_spec()] * 2,
        compiler_params=pltpu.CompilerParams(vmem_limit_bytes=24 << 20),
        name="attention",
    )(lengths, mine, peer, kv)


def project_kernel(n_cand, count, first_ref, second_ref, *refs):
    weights = refs[: 2 * n_cand]
    outs = refs[2 * n_cand : 2 * n_cand + count]
    own_s, par_s = refs[2 * n_cand + count :]
    share = first_ref.shape[0] // count
    core, chip, query_at = place(n_cand)
    straight = core == query_at
    for j in range(count):
        at = pl.multiple_of((chip ^ j) * share, share)
        to = slice(j * share, (j + 1) * share)
        first, second = first_ref[pl.ds(at, share), :], second_ref[pl.ds(at, share), :]
        own_s[to, :] = jnp.where(straight, first, second)
        par_s[to, :] = jnp.where(straight, second, first)
    own, par = own_s[...], par_s[...]
    width = weights[0].shape[1]
    for s in range(n_cand):
        block = dot32(own, weights[s][...]) + dot32(par, weights[n_cand + s][...])
        block = block.astype(jnp.bfloat16)
        for j in range(count):
            outs[j][:, s * width : (s + 1) * width] = block[j * share : (j + 1) * share, :]


def project(first, second, weights, count):
    rows, cols = first.shape
    n_cand = len(weights) // 2
    model = weights[0].shape[1] * n_cand
    return pl.pallas_call(
        functools.partial(project_kernel, n_cand, count),
        out_shape=[jax.ShapeDtypeStruct((rows // count, model), jnp.bfloat16)] * count,
        in_specs=[vmem_spec()] * (2 + len(weights)),
        out_specs=[vmem_spec()] * count,
        scratch_shapes=[VMEM((rows, cols), jnp.bfloat16)] * 2,
        compiler_params=pltpu.CompilerParams(vmem_limit_bytes=8 << 20),
        name="project",
    )(first, second, *weights)


def residual_kernel(count, n_cand, base_ref, gain_ref, *refs):
    total = base_ref[...].astype(jnp.float32)
    for part in refs[:count]:
        total = total + part[...].astype(jnp.float32)
    squares = jnp.mean(total * total, axis=-1, keepdims=True)
    scaled = total * lax.rsqrt(squares + NORM_EPS)
    block = base_ref.shape[1] // n_cand
    for s in range(n_cand):
        at = pl.multiple_of(lax.rem(lax.axis_index("cand") + s, n_cand) * block, block)
        to = slice(s * block, (s + 1) * block)
        refs[count][:, to] = (scaled[:, to] * gain_ref[:, pl.ds(at, block)]).astype(jnp.bfloat16)
    if len(refs) > count + 1:
        refs[count + 1][...] = total


def residual_norm(base, gain, parts, n_cand, keep):
    shapes = [jax.ShapeDtypeStruct(base.shape, jnp.bfloat16)]
    if keep:
        shapes.append(jax.ShapeDtypeStruct(base.shape, jnp.float32))
    return pl.pallas_call(
        functools.partial(residual_kernel, len(parts), n_cand),
        out_shape=shapes,
        in_specs=[vmem_spec()] * (2 + len(parts)),
        out_specs=[vmem_spec()] * len(shapes),
        compiler_params=pltpu.CompilerParams(vmem_limit_bytes=4 << 20),
        name="residual_norm",
    )(base, gain.reshape(1, -1), *parts)


def ffn_kernel(n_cand, count, *refs):
    n_w = 2 * n_cand
    rows_in = refs[:count]
    gates = refs[count : count + n_w]
    ups = refs[count + n_w : count + 2 * n_w]
    downs = refs[count + 2 * n_w : count + 3 * n_w]
    outs = refs[count + 3 * n_w : 2 * count + 3 * n_w]
    acts = refs[2 * count + 3 * n_w]
    share = rows_in[0].shape[0]
    for j in range(count):
        acts[j * share : (j + 1) * share, :] = rows_in[j][...]
    depth = gates[0].shape[1]
    hidden = []
    for side in range(2):
        gate_part, up_part = None, None
        for s in range(n_cand):
            i = side * n_cand + s
            block = acts[:, s * depth : (s + 1) * depth]
            term = dot32_t(gates[i][...], block)
            gate_part = term if gate_part is None else gate_part + term
            term = dot32_t(ups[i][...], block)
            up_part = term if up_part is None else up_part + term
        hidden.append((gelu_tanh(gate_part) * up_part).astype(jnp.bfloat16).T)
    width = downs[0].shape[1]
    for s in range(n_cand):
        block = dot32(hidden[0], downs[s][...]) + dot32(hidden[1], downs[n_cand + s][...])
        block = block.astype(jnp.bfloat16)
        for j in range(count):
            outs[j][:, s * width : (s + 1) * width] = block[j * share : (j + 1) * share, :]


def feed_forward(rows_in, gates, ups, downs):
    count, n_w = len(rows_in), len(gates)
    n_cand = n_w // 2
    share, model = rows_in[0].shape
    return pl.pallas_call(
        functools.partial(ffn_kernel, n_cand, count),
        out_shape=[jax.ShapeDtypeStruct((share, model), jnp.bfloat16)] * count,
        in_specs=[vmem_spec()] * (count + 3 * n_w),
        out_specs=[vmem_spec()] * count,
        scratch_shapes=[VMEM((share * count, model), jnp.bfloat16)],
        compiler_params=pltpu.CompilerParams(vmem_limit_bytes=24 << 20),
        name="feed_forward",
    )(*rows_in, *gates, *ups, *downs)


def vocab_kernel(n_cand, count, width, live, gold_ref, over_gold_ref, *refs):
    here, over = refs[:count], refs[count : 2 * count]
    own, swapped = refs[2 * count : 2 * count + n_cand], refs[2 * count + n_cand : -5]
    out_ref, acts, max_s, sum_s, gold_s = refs[-5:]
    share = here[0].shape[0]
    rows = 2 * count * share
    vocab, depth = own[0].shape
    core, chip, query_at = place(n_cand)
    mine = core == query_at
    start = (chip * 2 + query_at) * live
    gold_row = jnp.concatenate([gold_ref[...], over_gold_ref[...]], axis=1) - start
    for j in range(count):
        at = pl.multiple_of((chip ^ j) * share, share)
        acts[pl.ds(at, share), :] = here[j][...]
        for s in range(n_cand):
            p = (s - n_cand // 2) % n_cand
            acts[pl.ds(at + rows // 2, share), s * depth : (s + 1) * depth] = over[j][
                :, p * depth : (p + 1) * depth
            ]
    max_s[...] = jnp.full_like(max_s, NEG)
    sum_s[...] = jnp.zeros_like(sum_s)
    gold_s[...] = jnp.zeros_like(gold_s)
    for first in range(0, vocab, width):
        size = min(width, vocab - first)
        logits = None
        for s in range(n_cand):
            one, two = (own, swapped) if s == 0 else (swapped, own)
            at = slice(first, first + size)
            part = jnp.where(mine, one[s][at, :], two[s][at, :])
            term = dot32_t(part, acts[:, s * depth : (s + 1) * depth])
            logits = term if logits is None else logits + term
        column = first + lax.broadcasted_iota(jnp.int32, (size, 1), 0)
        hit = column == gold_row
        if first + size > live:
            hit = hit & (column < live)
            logits = jnp.where(column < live, logits, NEG)
        picked = jnp.where(hit, logits, 0.0)
        gold_s[...] += jnp.sum(picked.reshape(size // 8, 8, rows), axis=0)
        logits = logits.reshape(size // 8, 8, rows)
        old = max_s[...]
        new = jnp.maximum(old, jnp.max(logits, axis=0))
        terms = jnp.sum(jnp.exp(logits - new[None]), axis=0)
        sum_s[...] = sum_s[...] * jnp.exp(old - new) + terms
        max_s[...] = new
    top = jnp.max(max_s[...], axis=0, keepdims=True)
    total = jnp.sum(sum_s[...] * jnp.exp(max_s[...] - top), axis=0, keepdims=True)
    gold = jnp.sum(gold_s[...], axis=0, keepdims=True)
    for k, value in enumerate((top, total, gold)):
        for i in range(rows // 128):
            out_ref[k, i : i + 1, :] = value[:, i * 128 : (i + 1) * 128]


def vocab_scores(gold, over_gold, rows_in, own, swapped, live):
    count, n_cand = len(rows_in) // 2, len(own)
    share, model = rows_in[0].shape
    vocab = own[0].shape[0]
    rows = share * count * 2
    width = pl.cdiv(pl.cdiv(vocab, 3), 16) * 16
    assert rows % 256 == 0
    operands = (gold, over_gold, *rows_in, *own, *swapped)
    return pl.pallas_call(
        functools.partial(vocab_kernel, n_cand, count, width, live),
        out_shape=jax.ShapeDtypeStruct((3, rows // 128, 128), jnp.float32),
        in_specs=[vmem_spec()] * len(operands),
        out_specs=vmem_spec(),
        scratch_shapes=[VMEM((rows, model), jnp.bfloat16)] + [VMEM((8, rows), jnp.float32)] * 3,
        compiler_params=pltpu.CompilerParams(vmem_limit_bytes=20 << 20),
        name="vocab_scores",
    )(*operands)


def mean_kernel(length, n_cand, counts_ref, here_ref, there_ref, out_ref):
    core = place(n_cand)[0]
    cand = lax.axis_index("cand")
    middle = here_ref.shape[1] // 2
    sub = lax.broadcasted_iota(jnp.int32, (middle, 128), 0)
    row = sub * 128 + lax.broadcasted_iota(jnp.int32, (middle, 128), 1)
    lane = lax.broadcasted_iota(jnp.int32, (1, 128), 1)
    cands = middle * 128 // length
    best = jnp.full((1, 1), NEG, jnp.float32)
    for part in range(2):
        one, two = slice(part * middle, (part + 1) * middle), slice((1 - part) * middle, (2 - part) * middle)
        top_here, top_there = here_ref[0, one, :], there_ref[0, two, :]
        top = jnp.maximum(top_here, top_there)
        total = here_ref[1, one, :] * jnp.exp(top_here - top)
        total = total + there_ref[1, two, :] * jnp.exp(top_there - top)
        logprob = here_ref[2, one, :] + there_ref[2, two, :] - top - jnp.log(total)
        first = lax.rem(cand + part * (n_cand // 2), n_cand) * cands
        means = jnp.zeros((1, 128), jnp.float32)
        for c in range(cands):
            picked = jnp.where((row >= c * length) & (row < (c + 1) * length), logprob, 0.0)
            mean = jnp.sum(jnp.sum(picked, axis=0, keepdims=True), axis=1, keepdims=True) / length
            means = jnp.where(lane == c, mean, means)
            best = jnp.maximum(best, jnp.where(first + c < counts_ref[core], mean, NEG))
        if part == 0:
            own = means
    out_ref[...] = jnp.where(lane < cands, own, best)


def candidate_means(counts, here, there, length, n_cand):
    return pl.pallas_call(
        functools.partial(mean_kernel, length, n_cand),
        out_shape=jax.ShapeDtypeStruct((1, 128), jnp.float32),
        in_specs=[smem_spec(), vmem_spec(), vmem_spec()],
        out_specs=vmem_spec(),
        compiler_params=pltpu.CompilerParams(vmem_limit_bytes=2 << 20),
        name="candidate_means",
    )(counts, here, there)


def result_kernel(n_cand, counts_ref, here_ref, there_ref, scores_ref, best_ref):
    cands = scores_ref.shape[1]
    low = place(n_cand)[0] == 0
    here, there = here_ref[...], there_ref[...]
    lane = lax.broadcasted_iota(jnp.int32, (1, cands), 1) + lax.axis_index("cand") * cands
    for q in range(2):
        line = jnp.where(low, here, there) if q == 0 else jnp.where(low, there, here)
        scores_ref[q : q + 1, :] = jnp.where(lane < counts_ref[q], line[:, :cands], 0.0)
        best_ref[:, q : q + 1] = line[:, cands : cands + 1]


def results(counts, here, there, cands, n_cand):
    return pl.pallas_call(
        functools.partial(result_kernel, n_cand),
        out_shape=[
            jax.ShapeDtypeStruct((2, cands), jnp.float32),
            jax.ShapeDtypeStruct((1, 2), jnp.float32),
        ],
        in_specs=[smem_spec(), vmem_spec(), vmem_spec()],
        out_specs=[vmem_spec(), vmem_spec()],
        compiler_params=pltpu.CompilerParams(vmem_limit_bytes=2 << 20),
        name="results",
    )(counts, here, there)


def body(
    dec_hidden,
    enc_keys,
    enc_values,
    enc_lengths,
    cand_counts,
    gold_ids,
    gain_cross,
    w_query,
    w_out,
    gain_ffn,
    w_in_gate,
    w_in_up,
    w_ffn_out,
    gain_final,
    w_vocab,
):
    queries, cand_dev, length, model = dec_hidden.shape
    n_tok, n_cand = lax.axis_size("tok"), lax.axis_size("cand")
    tok, cand = lax.axis_index("tok"), lax.axis_index("cand")
    core, chip = tok % 2, tok // 2
    chips = n_tok // 2
    rows = cand_dev * length
    half = n_cand // 2
    share = rows // chips
    block = model // n_cand
    head_cols = w_query.shape[1]
    assert queries == 2 and n_cand % 2 == 0 and n_tok % 4 == 0 and n_tok & (n_tok - 1) == 0

    def swap(a, k):
        return lax.ppermute(a, "tok", [(i, i ^ k) for i in range(n_tok)])

    def across(a, shift):
        return lax.ppermute(a, "cand", [(i, (i - shift) % n_cand) for i in range(n_cand)])

    def from_cands(a):
        return [a] + [across(a, s) for s in range(1, n_cand)]

    def with_partner(parts):
        own = swap(parts[0], 1)
        return parts + [own] + [swap(a, 1) for a in parts[1:]]

    def rolled(a):
        return jnp.concatenate(
            [
                lax.dynamic_slice_in_dim(a, ((cand + s) % n_cand) * block, block, a.ndim - 1)
                for s in range(n_cand)
            ],
            axis=-1,
        )

    def gather_rows(a, both=False):
        out, over = [None] * chips, [None] * chips
        out[0] = a
        for j in range(2, chips, 2):
            out[j] = swap(a, 2 * j)
        for j in range(0, chips, 2):
            out[j + 1] = swap(out[j], 2)
        if not both:
            return out
        for j in range(chips):
            if j % 2 == 0 or j < 4:
                over[j] = across(out[j], half)
            else:
                over[j] = swap(over[j - 1], 2)
        return out + over

    def scatter_rows(parts):
        order = [j for j in range(4, chips, 2)] + [2, 0]
        near = {j: swap(parts[j + 1], 2) for j in order}
        back = [parts[0], near[0]]
        for j in order[:-1]:
            pair = parts[j].astype(jnp.float32) + near[j].astype(jnp.float32)
            back.append(swap(pair.astype(jnp.bfloat16), 2 * j))
        return back

    query_at = cand // half

    pair = by_heads(query_at, enc_keys, enc_values, n_tok, n_cand)
    key_values = lax.all_to_all(pair, "tok", 0, 0, tiled=True)

    query_parts = from_cands(w_query)
    out_parts = with_partner(from_cands(w_out))
    gate_parts = with_partner(from_cands(w_in_gate.T))
    up_parts = with_partner(from_cands(w_in_up.T))
    down_parts = with_partner(from_cands(w_ffn_out))
    vocab_dev = w_vocab.shape[1]
    vocab_own = w_vocab.T
    if vocab_dev % 8:
        vocab_own = jnp.pad(vocab_own, ((0, -vocab_dev % 8), (0, 0)))
    vocab_swapped = swap(vocab_own, 1)
    gold = lax.dynamic_index_in_dim(gold_ids, core, 0, keepdims=False).reshape(1, rows)
    over_gold = across(gold, half)

    flat = dec_hidden.reshape(queries * rows, model)
    flat, lengths = lax.optimization_barrier((flat, jnp.maximum(enc_lengths, 1)))
    base = rolled(lax.dynamic_slice_in_dim(flat, core * rows + chip * share, share, 0))
    flat = rolled(flat)
    wide = flat.astype(jnp.float32)
    gain_first = rolled(gain_cross.reshape(1, model))
    squares = jnp.mean(wide * wide, axis=-1, keepdims=True)
    normed = (wide * lax.rsqrt(squares + NORM_EPS) * gain_first).astype(jnp.bfloat16)
    query = sum(
        dot32(normed[:, s * block : (s + 1) * block], query_parts[s]) for s in range(n_cand)
    ).astype(jnp.bfloat16)
    query = query.reshape(queries, rows, head_cols)
    mine = lax.dynamic_index_in_dim(query, query_at, 0, keepdims=False)
    other = lax.dynamic_index_in_dim(query, 1 - query_at, 0, keepdims=False)
    peer = across(other, half)
    mine, base, gold, over_gold = lax.optimization_barrier((mine, base, gold, over_gold))
    first, second = attention(lengths, mine, peer, key_values, n_cand)

    def route(a, flip):
        perm = []
        for t in range(n_tok):
            for c in range(n_cand):
                to_half = (t % 2) ^ flip
                to = (t - t % 2 + c // half) * n_cand + c % half + to_half * half
                perm.append((t * n_cand + c, to))
        return lax.ppermute(a, ("tok", "cand"), perm)

    first, second = route(first, 0), route(second, 1)
    vocab_own = [vocab_own]
    for s in range(1, n_cand):
        perm = []
        for c in range(n_cand):
            side = c // half
            for t in range(0, n_tok, 2):
                perm.append(((t + side) * n_cand + (c + s) % n_cand, (t + 1 - side) * n_cand + c))
        vocab_own.append(lax.ppermute(vocab_own[0], ("tok", "cand"), perm))
    vocab_swapped = [vocab_swapped] + [swap(w, 1) for w in vocab_own[1:]]
    cross_terms = project(first, second, out_parts, chips)
    cross_terms = scatter_rows(cross_terms)
    normed_ffn, after_cross = residual_norm(base, gain_ffn, cross_terms, n_cand, True)
    ffn_rows = gather_rows(normed_ffn)
    ffn_terms = feed_forward(ffn_rows, gate_parts, up_parts, down_parts)
    ffn_terms = scatter_rows(ffn_terms)
    (normed_final,) = residual_norm(after_cross, gain_final, ffn_terms, n_cand, False)
    final_rows = gather_rows(normed_final, True)

    stats = vocab_scores(
        gold, over_gold, final_rows, vocab_own, vocab_swapped, vocab_dev
    )

    def combine(parts):
        top = functools.reduce(jnp.maximum, [p[0] for p in parts])
        total = sum(p[1] * jnp.exp(p[0] - top) for p in parts)
        return jnp.stack([top, total, sum(p[2] for p in parts)])

    stats = combine([stats, swap(stats, 2)])
    stats = combine([stats] + [swap(stats, 2 * j) for j in range(2, chips, 2)])
    theirs = across(stats, half)
    means = candidate_means(cand_counts, stats, theirs, length, n_cand)
    k = 1
    while k < half:
        other_best = lax.ppermute(means, "cand", [(i, i ^ k) for i in range(n_cand)])
        past = lax.iota(jnp.int32, 128)[None, :] >= cand_dev
        means = jnp.where(past, jnp.maximum(means, other_best), means)
        k *= 2
    cand_scores, best = results(cand_counts, means, swap(means, 1), cand_dev, n_cand)
    return (cand_scores, best.reshape(2))


def solution(mesh):
    in_specs = (
        P(None, "cand", None, None),
        P(None, "tok", None),
        P(None, "tok", None),
        P(),
        P(),
        P(None, "cand", None),
        P(),
        P("cand", "tok"),
        P("tok", "cand"),
        P(),
        P("cand", "tok"),
        P("cand", "tok"),
        P("tok", "cand"),
        P(),
        P("cand", "tok"),
    )
    out_specs = (P(None, "cand"), P())
    return jax.shard_map(body, mesh=mesh, in_specs=in_specs, out_specs=out_specs, check_vma=False)
```

```python
import functools

import jax
import jax.numpy as jnp
from jax import lax
from jax.experimental import pallas as pl
from jax.experimental.pallas import tpu as pltpu
from jax.sharding import PartitionSpec as P


HEAD_DIM = 64
NORM_EPS = 0.25
NEG = -1e30


VMEM = pltpu.VMEM
SMEM = pltpu.SMEM


def vmem_spec():
    return pl.BlockSpec(memory_space=VMEM)


def smem_spec():
    return pl.BlockSpec(memory_space=SMEM)


def hbm_spec():
    return pl.BlockSpec(memory_space=pltpu.MemorySpace.HBM)


def place(n_cand):
    tok = lax.axis_index("tok")
    return tok % 2, tok // 2, lax.axis_index("cand") // (n_cand // 2)


def dot32(a, b):
    return jnp.dot(a, b, preferred_element_type=jnp.float32)


def dot32_t(a, b):
    return lax.dot_general(a, b, (((1,), (1,)), ((), ())), preferred_element_type=jnp.float32)


def gelu_tanh(v):
    inner = 0.7978845608028654 * (v + 0.044715 * (v * v * v))
    return 0.5 * v * (1.0 + jnp.tanh(inner))


def by_heads_kernel(count, n_cand, keys_ref, values_ref, out_ref, sems):
    query_at = place(n_cand)[2]
    cols = out_ref.shape[3]
    copies = []
    for d in range(count):
        for k, ref in enumerate((keys_ref, values_ref)):
            copies.append(
                pltpu.make_async_copy(
                    ref.at[query_at, :, pl.ds(d * cols, cols)], out_ref.at[d, k], sems.at[d, k]
                )
            )
            copies[-1].start()
    for copy in copies:
        copy.wait()


def by_heads(query, keys, values, count, n_cand):
    src, model = keys.shape[1:]
    cols = model // count
    if cols % 128:
        pair = jnp.stack([lax.dynamic_index_in_dim(a, query, 0, False) for a in (keys, values)])
        return pair.reshape(2, src, count, cols).transpose(2, 0, 1, 3)
    return pl.pallas_call(
        functools.partial(by_heads_kernel, count, n_cand),
        out_shape=jax.ShapeDtypeStruct((count, 2, src, cols), keys.dtype),
        in_specs=[hbm_spec(), hbm_spec()],
        out_specs=vmem_spec(),
        scratch_shapes=[pltpu.SemaphoreType.DMA((count, 2))],
        compiler_params=pltpu.CompilerParams(vmem_limit_bytes=62 << 20),
        name="by_heads",
    )(keys, values)


def attention_kernel(n_cand, bias_ref, mine_ref, peer_ref, kv_ref, first_ref, second_ref):
    core, _, query_at = place(n_cand)
    straight = core == query_at
    src = kv_ref.shape[0] * kv_ref.shape[2]
    cols = kv_ref.shape[3]
    keys = kv_ref[:, 0].reshape(src, cols)
    values = kv_ref[:, 1].reshape(src, cols)
    bias = bias_ref[...]
    lane_head = lax.broadcasted_iota(jnp.int32, (1, cols), 1) // HEAD_DIM
    rows = mine_ref.shape[0]
    step = min(rows, 256)
    for out_ref, one_ref, two_ref in (
        (first_ref, mine_ref, peer_ref),
        (second_ref, peer_ref, mine_ref),
    ):
        for start in range(0, rows, step):
            at = slice(start, start + step)
            q = jnp.where(straight, one_ref[at, :], two_ref[at, :])
            mixed = jnp.zeros((step, cols), jnp.float32)
            for head in range(cols // HEAD_DIM):
                q_head = jnp.where(lane_head == head, q, jnp.zeros_like(q))
                scores = dot32_t(q_head, keys) + bias
                row_max = jnp.max(scores, axis=-1, keepdims=True)
                weights = jnp.exp(scores - row_max)
                denominator = jnp.sum(weights, axis=-1, keepdims=True)
                head_out = dot32(weights.astype(jnp.bfloat16), values) / denominator
                mixed = jnp.where(lane_head == head, head_out, mixed)
            out_ref[at, :] = mixed.astype(jnp.bfloat16)


def attention(bias, mine, peer, kv, n_cand):
    rows, cols = mine.shape
    return pl.pallas_call(
        functools.partial(attention_kernel, n_cand),
        out_shape=[jax.ShapeDtypeStruct((rows, cols), jnp.bfloat16)] * 2,
        in_specs=[vmem_spec()] * 4,
        out_specs=[vmem_spec()] * 2,
        compiler_params=pltpu.CompilerParams(vmem_limit_bytes=24 << 20),
        name="attention",
    )(bias, mine, peer, kv)


def project_kernel(n_cand, count, first_ref, second_ref, *refs):
    weights = refs[: 2 * n_cand]
    outs = refs[2 * n_cand : 2 * n_cand + count]
    own_s, par_s = refs[2 * n_cand + count :]
    share = first_ref.shape[0] // count
    core, chip, query_at = place(n_cand)
    straight = core == query_at
    for j in range(count):
        at = pl.multiple_of((chip ^ j) * share, share)
        to = slice(j * share, (j + 1) * share)
        first, second = first_ref[pl.ds(at, share), :], second_ref[pl.ds(at, share), :]
        own_s[to, :] = jnp.where(straight, first, second)
        par_s[to, :] = jnp.where(straight, second, first)
    own, par = own_s[...], par_s[...]
    width = weights[0].shape[1]
    for s in range(n_cand):
        block = dot32(own, weights[s][...]) + dot32(par, weights[n_cand + s][...])
        block = block.astype(jnp.bfloat16)
        for j in range(count):
            outs[j][:, s * width : (s + 1) * width] = block[j * share : (j + 1) * share, :]


def project(first, second, weights, count):
    rows, cols = first.shape
    n_cand = len(weights) // 2
    model = weights[0].shape[1] * n_cand
    return pl.pallas_call(
        functools.partial(project_kernel, n_cand, count),
        out_shape=[jax.ShapeDtypeStruct((rows // count, model), jnp.bfloat16)] * count,
        in_specs=[vmem_spec()] * (2 + len(weights)),
        out_specs=[vmem_spec()] * count,
        scratch_shapes=[VMEM((rows, cols), jnp.bfloat16)] * 2,
        compiler_params=pltpu.CompilerParams(vmem_limit_bytes=8 << 20),
        name="project",
    )(first, second, *weights)


def residual_kernel(count, which, base_ref, gains_ref, *refs):
    share = refs[0].shape[0]
    total = base_ref[:share, :].astype(jnp.float32)
    for part in refs[:count]:
        total = total + part[...].astype(jnp.float32)
    squares = jnp.mean(total * total, axis=-1, keepdims=True)
    gain = gains_ref[share + which : share + which + 1, :]
    refs[count][...] = (total * lax.rsqrt(squares + NORM_EPS) * gain).astype(jnp.bfloat16)
    if len(refs) > count + 1:
        refs[count + 1][...] = total


def residual_norm(base, gains, parts, which, keep):
    shapes = [jax.ShapeDtypeStruct(parts[0].shape, jnp.bfloat16)]
    if keep:
        shapes.append(jax.ShapeDtypeStruct(parts[0].shape, jnp.float32))
    return pl.pallas_call(
        functools.partial(residual_kernel, len(parts), which),
        out_shape=shapes,
        in_specs=[vmem_spec()] * (2 + len(parts)),
        out_specs=[vmem_spec()] * len(shapes),
        compiler_params=pltpu.CompilerParams(vmem_limit_bytes=4 << 20),
        name="residual_norm",
    )(base, gains, *parts)


def ffn_kernel(n_cand, count, *refs):
    n_w = 2 * n_cand
    rows_in = refs[:count]
    gates = refs[count : count + n_w]
    ups = refs[count + n_w : count + 2 * n_w]
    downs = refs[count + 2 * n_w : count + 3 * n_w]
    outs = refs[count + 3 * n_w : 2 * count + 3 * n_w]
    acts = refs[2 * count + 3 * n_w]
    share = rows_in[0].shape[0]
    for j in range(count):
        acts[j * share : (j + 1) * share, :] = rows_in[j][...]
    depth = gates[0].shape[1]
    hidden = []
    for side in range(2):
        gate_part, up_part = None, None
        for s in range(n_cand):
            i = side * n_cand + s
            block = acts[:, s * depth : (s + 1) * depth]
            term = dot32_t(gates[i][...], block)
            gate_part = term if gate_part is None else gate_part + term
            term = dot32_t(ups[i][...], block)
            up_part = term if up_part is None else up_part + term
        hidden.append((gelu_tanh(gate_part) * up_part).astype(jnp.bfloat16).T)
    width = downs[0].shape[1]
    for s in range(n_cand):
        block = dot32(hidden[0], downs[s][...]) + dot32(hidden[1], downs[n_cand + s][...])
        block = block.astype(jnp.bfloat16)
        for j in range(count):
            outs[j][:, s * width : (s + 1) * width] = block[j * share : (j + 1) * share, :]


def feed_forward(rows_in, gates, ups, downs):
    count, n_w = len(rows_in), len(gates)
    n_cand = n_w // 2
    share, model = rows_in[0].shape
    return pl.pallas_call(
        functools.partial(ffn_kernel, n_cand, count),
        out_shape=[jax.ShapeDtypeStruct((share, model), jnp.bfloat16)] * count,
        in_specs=[vmem_spec()] * (count + 3 * n_w),
        out_specs=[vmem_spec()] * count,
        scratch_shapes=[VMEM((share * count, model), jnp.bfloat16)],
        compiler_params=pltpu.CompilerParams(vmem_limit_bytes=24 << 20),
        name="feed_forward",
    )(*rows_in, *gates, *ups, *downs)


def vocab_kernel(n_cand, count, width, live, gold_ref, over_gold_ref, *refs):
    here, over = refs[:count], refs[count : 2 * count]
    own, swapped = refs[2 * count : 2 * count + n_cand], refs[2 * count + n_cand : -5]
    out_ref, acts, max_s, sum_s, gold_s = refs[-5:]
    share = here[0].shape[0]
    rows = 2 * count * share
    vocab, depth = own[0].shape
    core, chip, query_at = place(n_cand)
    mine = core == query_at
    start = (chip * 2 + query_at) * live
    gold_row = jnp.concatenate([gold_ref[...], over_gold_ref[...]], axis=1) - start
    for j in range(count):
        at = pl.multiple_of((chip ^ j) * share, share)
        acts[pl.ds(at, share), :] = here[j][...]
        for s in range(n_cand):
            p = (s - n_cand // 2) % n_cand
            acts[pl.ds(at + rows // 2, share), s * depth : (s + 1) * depth] = over[j][
                :, p * depth : (p + 1) * depth
            ]
    max_s[...] = jnp.full_like(max_s, NEG)
    sum_s[...] = jnp.zeros_like(sum_s)
    gold_s[...] = jnp.zeros_like(gold_s)
    for first in range(0, vocab, width):
        size = min(width, vocab - first)
        logits = None
        for s in range(n_cand):
            one, two = (own, swapped) if s == 0 else (swapped, own)
            at = slice(first, first + size)
            part = jnp.where(mine, one[s][at, :], two[s][at, :])
            term = dot32_t(part, acts[:, s * depth : (s + 1) * depth])
            logits = term if logits is None else logits + term
        column = first + lax.broadcasted_iota(jnp.int32, (size, 1), 0)
        hit = column == gold_row
        if first + size > live:
            hit = hit & (column < live)
            logits = jnp.where(column < live, logits, NEG)
        picked = jnp.where(hit, logits, 0.0)
        gold_s[...] += jnp.sum(picked.reshape(size // 8, 8, rows), axis=0)
        logits = logits.reshape(size // 8, 8, rows)
        old = max_s[...]
        new = jnp.maximum(old, jnp.max(logits, axis=0))
        terms = jnp.sum(jnp.exp(logits - new[None]), axis=0)
        sum_s[...] = sum_s[...] * jnp.exp(old - new) + terms
        max_s[...] = new
    top = jnp.max(max_s[...], axis=0, keepdims=True)
    total = jnp.sum(sum_s[...] * jnp.exp(max_s[...] - top), axis=0, keepdims=True)
    gold = jnp.sum(gold_s[...], axis=0, keepdims=True)
    for k, value in enumerate((top, total, gold)):
        for i in range(rows // 128):
            out_ref[k, i : i + 1, :] = value[:, i * 128 : (i + 1) * 128]


def vocab_scores(gold, over_gold, rows_in, own, swapped, live):
    count, n_cand = len(rows_in) // 2, len(own)
    share, model = rows_in[0].shape
    vocab = own[0].shape[0]
    rows = share * count * 2
    width = pl.cdiv(pl.cdiv(vocab, 3), 16) * 16
    assert rows % 256 == 0
    operands = (gold, over_gold, *rows_in, *own, *swapped)
    return pl.pallas_call(
        functools.partial(vocab_kernel, n_cand, count, width, live),
        out_shape=jax.ShapeDtypeStruct((3, rows // 128, 128), jnp.float32),
        in_specs=[vmem_spec()] * len(operands),
        out_specs=vmem_spec(),
        scratch_shapes=[VMEM((rows, model), jnp.bfloat16)] + [VMEM((8, rows), jnp.float32)] * 3,
        compiler_params=pltpu.CompilerParams(vmem_limit_bytes=20 << 20),
        name="vocab_scores",
    )(*operands)


def mean_kernel(length, n_cand, counts_ref, here_ref, there_ref, out_ref):
    core = place(n_cand)[0]
    cand = lax.axis_index("cand")
    middle = here_ref.shape[1] // 2
    sub = lax.broadcasted_iota(jnp.int32, (middle, 128), 0)
    row = sub * 128 + lax.broadcasted_iota(jnp.int32, (middle, 128), 1)
    lane = lax.broadcasted_iota(jnp.int32, (1, 128), 1)
    cands = middle * 128 // length
    best = jnp.full((1, 1), NEG, jnp.float32)
    for part in range(2):
        one, two = slice(part * middle, (part + 1) * middle), slice((1 - part) * middle, (2 - part) * middle)
        top_here, top_there = here_ref[0, one, :], there_ref[0, two, :]
        top = jnp.maximum(top_here, top_there)
        total = here_ref[1, one, :] * jnp.exp(top_here - top)
        total = total + there_ref[1, two, :] * jnp.exp(top_there - top)
        logprob = here_ref[2, one, :] + there_ref[2, two, :] - top - jnp.log(total)
        first = lax.rem(cand + part * (n_cand // 2), n_cand) * cands
        means = jnp.zeros((1, 128), jnp.float32)
        for c in range(cands):
            picked = jnp.where((row >= c * length) & (row < (c + 1) * length), logprob, 0.0)
            mean = jnp.sum(jnp.sum(picked, axis=0, keepdims=True), axis=1, keepdims=True) / length
            means = jnp.where(lane == c, mean, means)
            best = jnp.maximum(best, jnp.where(first + c < counts_ref[core], mean, NEG))
        if part == 0:
            own = means
    out_ref[...] = jnp.where(lane < cands, own, best)


def candidate_means(counts, here, there, length, n_cand):
    return pl.pallas_call(
        functools.partial(mean_kernel, length, n_cand),
        out_shape=jax.ShapeDtypeStruct((1, 128), jnp.float32),
        in_specs=[smem_spec(), vmem_spec(), vmem_spec()],
        out_specs=vmem_spec(),
        compiler_params=pltpu.CompilerParams(vmem_limit_bytes=2 << 20),
        name="candidate_means",
    )(counts, here, there)


def result_kernel(n_cand, counts_ref, here_ref, there_ref, scores_ref, best_ref):
    cands = scores_ref.shape[1]
    low = place(n_cand)[0] == 0
    here, there = here_ref[...], there_ref[...]
    lane = lax.broadcasted_iota(jnp.int32, (1, cands), 1) + lax.axis_index("cand") * cands
    for q in range(2):
        line = jnp.where(low, here, there) if q == 0 else jnp.where(low, there, here)
        scores_ref[q : q + 1, :] = jnp.where(lane < counts_ref[q], line[:, :cands], 0.0)
        best_ref[:, q : q + 1] = line[:, cands : cands + 1]


def results(counts, here, there, cands, n_cand):
    return pl.pallas_call(
        functools.partial(result_kernel, n_cand),
        out_shape=[
            jax.ShapeDtypeStruct((2, cands), jnp.float32),
            jax.ShapeDtypeStruct((1, 2), jnp.float32),
        ],
        in_specs=[smem_spec(), vmem_spec(), vmem_spec()],
        out_specs=[vmem_spec(), vmem_spec()],
        compiler_params=pltpu.CompilerParams(vmem_limit_bytes=2 << 20),
        name="results",
    )(counts, here, there)


def body(
    dec_hidden,
    enc_keys,
    enc_values,
    enc_lengths,
    cand_counts,
    gold_ids,
    gain_cross,
    w_query,
    w_out,
    gain_ffn,
    w_in_gate,
    w_in_up,
    w_ffn_out,
    gain_final,
    w_vocab,
):
    queries, cand_dev, length, model = dec_hidden.shape
    n_tok, n_cand = lax.axis_size("tok"), lax.axis_size("cand")
    tok, cand = lax.axis_index("tok"), lax.axis_index("cand")
    core, chip = tok % 2, tok // 2
    chips = n_tok // 2
    rows = cand_dev * length
    half = n_cand // 2
    share = rows // chips
    block = model // n_cand
    head_cols = w_query.shape[1]
    assert queries == 2 and n_cand % 2 == 0 and n_tok % 4 == 0 and n_tok & (n_tok - 1) == 0

    def swap(a, k):
        return lax.ppermute(a, "tok", [(i, i ^ k) for i in range(n_tok)])

    def across(a, shift):
        return lax.ppermute(a, "cand", [(i, (i - shift) % n_cand) for i in range(n_cand)])

    def from_cands(a):
        return [a] + [across(a, s) for s in range(1, n_cand)]

    def with_partner(parts):
        own = swap(parts[0], 1)
        return parts + [own] + [swap(a, 1) for a in parts[1:]]

    def rolled(a):
        return jnp.concatenate(
            [
                lax.dynamic_slice_in_dim(a, ((cand + s) % n_cand) * block, block, a.ndim - 1)
                for s in range(n_cand)
            ],
            axis=-1,
        )

    def gather_rows(a, both=False):
        out, over = [None] * chips, [None] * chips
        out[0] = a
        for j in range(2, chips, 2):
            out[j] = swap(a, 2 * j)
        for j in range(0, chips, 2):
            out[j + 1] = swap(out[j], 2)
        if not both:
            return out
        for j in range(chips):
            if j % 2 == 0 or j < 4:
                over[j] = across(out[j], half)
            else:
                over[j] = swap(over[j - 1], 2)
        return out + over

    def scatter_rows(parts):
        order = [j for j in range(4, chips, 2)] + [2, 0]
        near = {j: swap(parts[j + 1], 2) for j in order}
        back = [parts[0], near[0]]
        for j in order[:-1]:
            pair = parts[j].astype(jnp.float32) + near[j].astype(jnp.float32)
            back.append(swap(pair.astype(jnp.bfloat16), 2 * j))
        return back

    query_at = cand // half

    pair = by_heads(query_at, enc_keys, enc_values, n_tok, n_cand)
    key_values = lax.all_to_all(pair, "tok", 0, 0, tiled=True)

    query_parts = from_cands(w_query)
    out_parts = with_partner(from_cands(w_out))
    gate_parts = with_partner(from_cands(w_in_gate.T))
    up_parts = with_partner(from_cands(w_in_up.T))
    down_parts = with_partner(from_cands(w_ffn_out))
    vocab_dev = w_vocab.shape[1]
    vocab_own = w_vocab.T
    if vocab_dev % 8:
        vocab_own = jnp.pad(vocab_own, ((0, -vocab_dev % 8), (0, 0)))
    vocab_swapped = swap(vocab_own, 1)
    gold = lax.dynamic_index_in_dim(gold_ids, core, 0, keepdims=False).reshape(1, rows)
    over_gold = across(gold, half)

    flat = dec_hidden.reshape(queries * rows, model)
    token = lax.iota(jnp.int32, enc_keys.shape[1] * n_tok)[None, :]
    length_here = lax.dynamic_index_in_dim(enc_lengths, query_at, 0, keepdims=False)
    bias = jnp.where(token < length_here, 0.0, NEG).astype(jnp.float32)
    flat, bias = lax.optimization_barrier((flat, bias))
    base = rolled(lax.dynamic_slice_in_dim(flat, core * rows + chip * share, share, 0))
    base = jnp.concatenate(
        [base.astype(jnp.float32)]
        + [rolled(gain.reshape(1, model)) for gain in (gain_ffn, gain_final)]
    )
    flat = rolled(flat)
    wide = flat.astype(jnp.float32)
    gain_first = rolled(gain_cross.reshape(1, model))
    squares = jnp.mean(wide * wide, axis=-1, keepdims=True)
    normed = (wide * lax.rsqrt(squares + NORM_EPS) * gain_first).astype(jnp.bfloat16)
    query = sum(
        dot32(normed[:, s * block : (s + 1) * block], query_parts[s]) for s in range(n_cand)
    ).astype(jnp.bfloat16)
    query = query.reshape(queries, rows, head_cols)
    mine = lax.dynamic_index_in_dim(query, query_at, 0, keepdims=False)
    other = lax.dynamic_index_in_dim(query, 1 - query_at, 0, keepdims=False)
    peer = across(other, half)
    mine, base, gold, over_gold = lax.optimization_barrier((mine, base, gold, over_gold))
    first, second = attention(bias, mine, peer, key_values, n_cand)

    def route(a, flip):
        perm = []
        for t in range(n_tok):
            for c in range(n_cand):
                to_half = (t % 2) ^ flip
                to = (t - t % 2 + c // half) * n_cand + c % half + to_half * half
                perm.append((t * n_cand + c, to))
        return lax.ppermute(a, ("tok", "cand"), perm)

    first, second = route(first, 0), route(second, 1)
    vocab_own = [vocab_own]
    for s in range(1, n_cand):
        perm = []
        for c in range(n_cand):
            side = c // half
            for t in range(0, n_tok, 2):
                perm.append(((t + side) * n_cand + (c + s) % n_cand, (t + 1 - side) * n_cand + c))
        vocab_own.append(lax.ppermute(vocab_own[0], ("tok", "cand"), perm))
    vocab_swapped = [vocab_swapped] + [swap(w, 1) for w in vocab_own[1:]]
    cross_terms = project(first, second, out_parts, chips)
    cross_terms = scatter_rows(cross_terms)
    normed_ffn, after_cross = residual_norm(base, base, cross_terms, 0, True)
    ffn_rows = gather_rows(normed_ffn)
    ffn_terms = feed_forward(ffn_rows, gate_parts, up_parts, down_parts)
    ffn_terms = scatter_rows(ffn_terms)
    (normed_final,) = residual_norm(after_cross, base, ffn_terms, 1, False)
    final_rows = gather_rows(normed_final, True)

    stats = vocab_scores(
        gold, over_gold, final_rows, vocab_own, vocab_swapped, vocab_dev
    )

    def combine(parts):
        top = functools.reduce(jnp.maximum, [p[0] for p in parts])
        total = sum(p[1] * jnp.exp(p[0] - top) for p in parts)
        return jnp.stack([top, total, sum(p[2] for p in parts)])

    stats = combine([stats, swap(stats, 2)])
    stats = combine([stats] + [swap(stats, 2 * j) for j in range(2, chips, 2)])
    theirs = across(stats, half)
    means = candidate_means(cand_counts, stats, theirs, length, n_cand)
    k = 1
    while k < half:
        other_best = lax.ppermute(means, "cand", [(i, i ^ k) for i in range(n_cand)])
        past = lax.iota(jnp.int32, 128)[None, :] >= cand_dev
        means = jnp.where(past, jnp.maximum(means, other_best), means)
        k *= 2
    cand_scores, best = results(cand_counts, means, swap(means, 1), cand_dev, n_cand)
    return (cand_scores, best.reshape(2))


def solution(mesh):
    in_specs = (
        P(None, "cand", None, None),
        P(None, "tok", None),
        P(None, "tok", None),
        P(),
        P(),
        P(None, "cand", None),
        P(),
        P("cand", "tok"),
        P("tok", "cand"),
        P(),
        P("cand", "tok"),
        P("cand", "tok"),
        P("tok", "cand"),
        P(),
        P("cand", "tok"),
    )
    out_specs = (P(None, "cand"), P())
    return jax.shard_map(body, mesh=mesh, in_specs=in_specs, out_specs=out_specs, check_vma=False)
```
